256 devices in a mesh: gx: 8 (over z), gy: 8 (over y, core), gz: 4 (over x).
Axes of the slice: x: 4, y: 4, z: 8, core: 2. Of those that a mesh axis runs over, the one named last changes fastest.
Arguments:
- acts: bfloat16 [150528, 2048], P(('gx', 'gy', 'gz')), may hold values from -24 to 24
- saved_hidden: bfloat16 [150528, 512], P(('gx', 'gy', 'gz')), as said below
- grad_out: bfloat16 [150528, 2048], P(('gx', 'gy', 'gz')), may hold values from -24 to 24
- master_reduce: float32 [2048, 512], P(('gx', 'gy', 'gz')), may hold values from -60 to 60
- master_expand: float32 [2048, 512], P(('gx', 'gy', 'gz')), may hold values from -60 to 60
- velocity_reduce: float32 [2048, 512], P(('gx', 'gy', 'gz')), may hold values from -6 to 6
- velocity_expand: float32 [2048, 512], P(('gx', 'gy', 'gz')), may hold values from -6 to 6
Outputs:
- grad_in: bfloat16 [150528, 2048], P(('gx', 'gy', 'gz'))
- new_master_reduce: float32 [2048, 512], P(('gx', 'gy', 'gz'))
- new_master_expand: float32 [2048, 512], P(('gx', 'gy', 'gz'))
- new_velocity_reduce: float32 [2048, 512], P(('gx', 'gy', 'gz'))
- new_velocity_expand: float32 [2048, 512], P(('gx', 'gy', 'gz'))
- work_reduce: bfloat16 [2048, 512], replicated
- work_expand: bfloat16 [2048, 512], replicated
The draws below stay inside these ranges and needn't reach their ends.
Inputs may be any that keep to these rules, and one draw needn't show every extreme that they name: `saved_hidden`: values are zero or positive, zero at about half of the entries.
All inputs are finite; a program needn't handle non-finite values.
Results may differ from the reference program's by a relative error of at most 0.0064.
Values may be sent and summed in bfloat16 or wider, within the bound.
No kernel may reach another device: no remote copies, remote signals or barrier semaphores. Data moves between devices by JAX's collectives and lax.ppermute only.
A program may use at most 64 MiB of HBM per device.

```python
import jax
import jax.numpy as jnp
from jax import lax

CHANNELS = 2048
MIDDLE = 512
ROWS = 150528


def draw_saved_hidden(key, part):
    values = jax.random.normal(jax.random.fold_in(key, 11), (ROWS, MIDDLE), jnp.float32)
    return jnp.maximum(values, 0.0).astype(jnp.bfloat16)


def rising_master(key, salt):
    values = jnp.clip(jax.random.normal(jax.random.fold_in(key, salt), (CHANNELS, MIDDLE), jnp.float32), -6.0, 6.0)
    place = jnp.arange(CHANNELS, dtype=jnp.float32)[:, None] / float(max(CHANNELS - 1, 1))
    scales = 1.0 + 2.0 * place
    return values * scales


def draw_master_reduce(key, part):
    return rising_master(key, 21)


def draw_master_expand(key, part):
    return rising_master(key, 31)


def strengthened(entries, stream_key, source, target, shards_of, factor):
    owner, partner = [(jnp.arange(entries.shape[dim]) // (entries.shape[dim] // shards_of)).reshape([-1 if axis == dim else 1 for axis in range(entries.ndim)]) for dim in (source, target)]
    chosen = jax.random.permutation(stream_key, shards_of)[partner]
    strong = (owner == chosen) | (owner == (partner + shards_of // 2) % shards_of)
    return jnp.where(strong, factor * entries, entries)


def levels(key, extent, cuts, least, high):
    def one(dim, shards_of):
        steps = jax.random.uniform(jax.random.fold_in(jax.random.fold_in(key, 6), dim), (shards_of,), jnp.float32, least / len(cuts), high / len(cuts))
        return jnp.repeat(jnp.exp(steps), extent[dim] // shards_of).reshape((-1,) + (1,) * (len(extent) - dim - 1))

    level = one(*cuts[0])
    for cut in cuts[1:]:
        level = level * one(*cut)
    return level


def gaussian(rng, dims, deviation, most, cuts=(), held_as=jnp.bfloat16):
    level = levels(rng, dims, cuts, -0.22, 0.18) if cuts else 1.0
    entries = jax.random.normal(rng, dims, jnp.float32) * deviation * level
    return jnp.minimum(jnp.maximum(entries, -most), most).astype(held_as)


def gaussian_with(rng, extent, scale, most, split, heavy, held_as=jnp.bfloat16):
    drawn = scale * jax.random.normal(rng, extent, jnp.float32)
    if split:
        drawn = drawn * levels(rng, extent, split, -0.22, 0.18)
    return jnp.clip(strengthened(drawn, jax.random.fold_in(rng, 3), *heavy), -most, most).astype(held_as)


def setup_inputs(seed: int = 0) -> dict:
    key_list = jax.random.split(jax.random.key(seed), 8)
    return {
        "acts": gaussian_with(key_list[0], (ROWS, CHANNELS), 1.0, 24.0, ((0, 256),), (0, 1, 256, 6.0)),
        "saved_hidden": draw_saved_hidden(jax.random.fold_in(key_list[7], 71), 0),
        "grad_out": gaussian_with(key_list[2], (ROWS, CHANNELS), 1.0, 24.0, ((0, 256),), (0, 1, 256, 6.0)),
        "master_reduce": draw_master_reduce(jax.random.fold_in(key_list[7], 71), 0),
        "master_expand": draw_master_expand(jax.random.fold_in(key_list[7], 71), 0),
        "velocity_reduce": gaussian(key_list[5], (CHANNELS, MIDDLE), 1.0, 6.0, ((0, 256),), jnp.float32),
        "velocity_expand": gaussian(key_list[6], (CHANNELS, MIDDLE), 1.0, 6.0, ((0, 256),), jnp.float32),
    }


def layer_update(master, grads, velocity):
    wnorm = jnp.sqrt(jnp.sum(master * master))
    gnorm = jnp.sqrt(jnp.sum(grads * grads))
    trust = wnorm / (gnorm + 5e-05 * wnorm)
    new_velocity = 0.9 * velocity + trust * (grads + 5e-05 * master)
    new_master = master - 0.1 * new_velocity
    return (new_master, new_velocity, new_master.astype(jnp.bfloat16))

def reference(acts, saved_hidden, grad_out, master_reduce, master_expand, velocity_reduce, velocity_expand):
    inv_c = 1.0 / math_sqrt(CHANNELS)
    inv_m = 1.0 / math_sqrt(MIDDLE)
    cur_reduce = master_reduce.astype(jnp.bfloat16)
    cur_expand = master_expand.astype(jnp.bfloat16)
    summed = jnp.dot(grad_out, cur_expand, preferred_element_type=jnp.float32)
    grad_hidden = jnp.where(saved_hidden > 0, summed * inv_m, 0.0).astype(jnp.bfloat16)
    g_expand = lax.dot_general(grad_out, saved_hidden, (((0,), (0,)), ((), ())), preferred_element_type=jnp.float32) * inv_m
    g_reduce = lax.dot_general(acts, grad_hidden, (((0,), (0,)), ((), ())), preferred_element_type=jnp.float32) * inv_c
    back = lax.dot_general(grad_hidden, cur_reduce, (((1,), (1,)), ((), ())), preferred_element_type=jnp.float32)
    grad_in = (grad_out.astype(jnp.float32) + back * inv_c).astype(jnp.bfloat16)
    new_mr, new_vr, work_reduce = layer_update(master_reduce, g_reduce, velocity_reduce)
    new_me, new_ve, work_expand = layer_update(master_expand, g_expand, velocity_expand)
    return (grad_in, new_mr, new_me, new_vr, new_ve, work_reduce, work_expand)

def math_sqrt(value):
    return float(value) ** 0.5
```

```python
import jax
import jax.numpy as jnp
from jax import lax
from jax.sharding import Mesh
from jax.sharding import PartitionSpec as P

ROWS_OVER = ("z", "y", "c", "x")
BF = jnp.bfloat16
F32 = jnp.float32


def exchange(parts, axes):
    return lax.all_to_all(parts, axes, 0, 0, tiled=True)


def everywhere(block, axes):
    peers = lax.axis_size(axes)
    return exchange(jnp.broadcast_to(block[None], (peers, *block.shape)), axes)


def from_other_core(block):
    return lax.ppermute(block, "c", [(0, 1), (1, 0)])


def both_cores(block):
    core = lax.axis_index("c")
    other = from_other_core(block)
    first = jnp.where(core == 0, block, other)
    second = jnp.where(core == 0, other, block)
    return jnp.stack([first, second])


def whole_rows(parts, rest):
    c, yx, z, r, n = parts.shape
    parts = parts.reshape(c, 4, 4, z, r, n)
    return parts.transpose(3, 1, 0, 2, 4, 5).reshape(c * yx * z * r, n)


def core_half(terms):
    rows, n = terms.shape
    parts = terms.astype(BF).reshape(8, 4, 2, 4, rows // 256, n)
    core = lax.axis_index("c")
    mine = lax.dynamic_index_in_dim(parts, core, 2, keepdims=False)
    others = lax.dynamic_index_in_dim(parts, 1 - core, 2, keepdims=False)
    got = from_other_core(others)
    both = mine.astype(F32) + got.astype(F32)
    return both.astype(BF).transpose(1, 2, 0, 3, 4).reshape(16, 8, rows // 256, n)


def layer_update(master, grads, velocity, wsquare, gsquare):
    wnorm = jnp.sqrt(wsquare)
    gnorm = jnp.sqrt(gsquare)
    trust = wnorm / (gnorm + 5e-05 * wnorm)
    new_velocity = 0.9 * velocity + trust * (grads + 5e-05 * master)
    new_master = master - 0.1 * new_velocity
    return (new_master, new_velocity)


def shards(
    acts, saved_hidden, grad_out, master_reduce, master_expand, velocity_reduce, velocity_expand
):
    channels = grad_out.shape[1]
    middle = saved_hidden.shape[1]
    inv_c = 1.0 / float(channels) ** 0.5
    inv_m = 1.0 / float(middle) ** 0.5
    cur = jnp.stack([master_expand.astype(BF), master_reduce.astype(BF)])
    along_z = everywhere(cur, "z")
    expand_parts = everywhere(along_z[:, 0], ("y", "x"))
    cur_expand = whole_rows(both_cores(expand_parts), middle)
    reduce_parts = everywhere(along_z[:, 1], ("y", "x"))
    g_expand_half = core_half(
        lax.dot_general(
            grad_out, saved_hidden, (((0,), (0,)), ((), ())), preferred_element_type=F32
        )
        * inv_m
    )
    summed = jnp.dot(grad_out, cur_expand, preferred_element_type=F32)
    grad_hidden = jnp.where(saved_hidden > 0, summed * inv_m, 0.0).astype(BF)
    g_reduce_half = core_half(
        lax.dot_general(acts, grad_hidden, (((0,), (0,)), ((), ())), preferred_element_type=F32)
        * inv_c
    )
    halves = jnp.stack([g_expand_half, g_reduce_half], axis=1)
    arrived = exchange(halves, ("y", "x"))
    over_plane = jnp.sum(arrived.astype(F32), axis=0).astype(BF)
    arrived = exchange(over_plane.transpose(1, 0, 2, 3), "z")
    grads = jnp.sum(arrived.astype(F32), axis=0)
    g_expand, g_reduce = grads[0], grads[1]

    cur_reduce = whole_rows(both_cores(reduce_parts), middle)
    back = lax.dot_general(
        grad_hidden, cur_reduce, (((1,), (1,)), ((), ())), preferred_element_type=F32
    )
    grad_in = (grad_out.astype(F32) + back * inv_c).astype(BF)

    squares = jnp.stack(
        [
            jnp.sum(master_expand * master_expand),
            jnp.sum(g_expand * g_expand),
            jnp.sum(master_reduce * master_reduce),
            jnp.sum(g_reduce * g_reduce),
        ]
    )
    squares = everywhere(squares[None], ("z", "y")).sum(axis=0)
    squares = everywhere(squares, ("c", "x")).sum(axis=0)[0]
    new_mr, new_vr = layer_update(master_reduce, g_reduce, velocity_reduce, squares[2], squares[3])
    new_me, new_ve = layer_update(master_expand, g_expand, velocity_expand, squares[0], squares[1])
    work = jnp.stack([new_me.astype(BF), new_mr.astype(BF)])
    along_z = everywhere(work, "z")
    parts = both_cores(everywhere(along_z, ("y", "x")))
    work_expand = whole_rows(parts[:, :, :, 0], middle)
    work_reduce = whole_rows(parts[:, :, :, 1], middle)
    return (grad_in, new_mr, new_me, new_vr, new_ve, work_reduce, work_expand)


def solution(mesh):
    finer = Mesh(mesh.devices.reshape(8, 4, 2, 4), ROWS_OVER)
    split = P(ROWS_OVER, None)
    return jax.shard_map(
        shards,
        mesh=finer,
        in_specs=(split,) * 7,
        out_specs=(split,) * 5 + (P(), P()),
        check_vma=False,
    )
```

```python
import jax
import jax.numpy as jnp
from jax import lax
from jax.sharding import Mesh
from jax.sharding import PartitionSpec as P


ROWS_OVER = ("z", "y", "c", "x")
BF = jnp.bfloat16
F32 = jnp.float32


def exchange(parts, axes):
    return lax.all_to_all(parts, axes, 0, 0, tiled=True)


def everywhere(block, axes):
    peers = lax.axis_size(axes)
    return exchange(jnp.broadcast_to(block[None], (peers, *block.shape)), axes)


def from_other_core(block):
    return lax.ppermute(block, "c", [(0, 1), (1, 0)])


def both_cores(block):
    core = lax.axis_index("c")
    other = from_other_core(block)
    first = jnp.where(core == 0, block, other)
    second = jnp.where(core == 0, other, block)
    return jnp.stack([first, second])


def whole_rows(parts):
    c, yx, z, r, n = parts.shape
    parts = parts.reshape(c, 4, 4, z, r, n)
    return parts.transpose(3, 1, 0, 2, 4, 5).reshape(c * yx * z * r, n)


def core_half(terms):
    rows, n = terms.shape
    parts = terms.reshape(8, 4, 2, 4, rows // 256, n)
    core = lax.axis_index("c")
    mine = lax.dynamic_index_in_dim(parts, core, 2, keepdims=False)
    others = lax.dynamic_index_in_dim(parts, 1 - core, 2, keepdims=False)
    got = from_other_core(others)
    both = mine.astype(F32) + got.astype(F32)
    return both.astype(BF).transpose(1, 2, 0, 3, 4).reshape(16, 8, rows // 256, n)


def layer_update(master, grads, velocity, wsquare, gsquare):
    wnorm = jnp.sqrt(wsquare)
    gnorm = jnp.sqrt(gsquare)
    trust = wnorm / (gnorm + 5e-05 * wnorm)
    new_velocity = 0.9 * velocity + trust * (grads + 5e-05 * master)
    new_master = master - 0.1 * new_velocity
    return (new_master, new_velocity)


def step(
    acts, saved_hidden, grad_out, master_reduce, master_expand, velocity_reduce, velocity_expand
):
    channels = grad_out.shape[1]
    middle = saved_hidden.shape[1]
    inv_c = 1.0 / float(channels) ** 0.5
    inv_m = 1.0 / float(middle) ** 0.5
    cur = jnp.stack([master_expand.astype(BF), master_reduce.astype(BF)])
    along_z = everywhere(cur, "z")
    expand_parts = everywhere(along_z[:, 0], ("y", "x"))
    cur_expand = whole_rows(both_cores(expand_parts))
    reduce_parts = everywhere(along_z[:, 1], ("y", "x"))
    expand_terms = (
        lax.dot_general(
            grad_out, saved_hidden, (((0,), (0,)), ((), ())), preferred_element_type=F32
        )
        * inv_m
    ).astype(BF)
    g_expand_half = core_half(expand_terms)
    summed = jnp.dot(grad_out, cur_expand, preferred_element_type=F32)
    grad_hidden = jnp.where(saved_hidden > 0, summed * inv_m, 0.0).astype(BF)
    reduce_terms = (
        lax.dot_general(
            acts, grad_hidden, (((0,), (0,)), ((), ())), preferred_element_type=F32
        )
        * inv_c
    ).astype(BF)
    g_reduce_half = core_half(reduce_terms)
    halves = jnp.stack([g_expand_half, g_reduce_half], axis=1)
    halves, reduce_parts = lax.optimization_barrier((halves, reduce_parts))
    arrived = exchange(halves, ("y", "x"))
    over_plane = jnp.sum(arrived.astype(F32), axis=0).astype(BF)
    arrived = exchange(over_plane.transpose(1, 0, 2, 3), "z")
    grads = jnp.sum(arrived.astype(F32), axis=0)
    g_expand, g_reduce = grads[0], grads[1]

    cur_reduce = whole_rows(both_cores(reduce_parts))
    back = lax.dot_general(
        grad_hidden, cur_reduce, (((1,), (1,)), ((), ())), preferred_element_type=F32
    )
    grad_in = (grad_out.astype(F32) + back * inv_c).astype(BF)

    squares = jnp.stack(
        [
            jnp.sum(master_expand * master_expand),
            jnp.sum(g_expand * g_expand),
            jnp.sum(master_reduce * master_reduce),
            jnp.sum(g_reduce * g_reduce),
        ]
    )
    squares = everywhere(squares[None], ("z", "y")).sum(axis=0)
    squares = everywhere(squares, ("c", "x")).sum(axis=0)[0]
    new_mr, new_vr = layer_update(master_reduce, g_reduce, velocity_reduce, squares[2], squares[3])
    new_me, new_ve = layer_update(master_expand, g_expand, velocity_expand, squares[0], squares[1])
    work = jnp.stack([new_me.astype(BF), new_mr.astype(BF)])
    along_z = everywhere(work, "z")
    parts = both_cores(everywhere(along_z, ("y", "x")))
    work_expand = whole_rows(parts[:, :, :, 0])
    work_reduce = whole_rows(parts[:, :, :, 1])
    return (grad_in, new_mr, new_me, new_vr, new_ve, work_reduce, work_expand)


def solution(mesh):
    finer = Mesh(mesh.devices.reshape(8, 4, 2, 4), ROWS_OVER)
    split = P(ROWS_OVER, None)
    return jax.shard_map(
        step,
        mesh=finer,
        in_specs=(split,) * 7,
        out_specs=(split,) * 5 + (P(), P()),
        check_vma=False,
    )
```

```python
import functools

import jax
import jax.numpy as jnp
from jax import lax
from jax.experimental import pallas as pl
from jax.experimental.pallas import tpu as pltpu
from jax.sharding import Mesh
from jax.sharding import PartitionSpec as P


ROWS_OVER = ("z", "y", "c", "x")
BF = jnp.bfloat16
F32 = jnp.float32


def exchange(parts, axes):
    return lax.all_to_all(parts, axes, 0, 0, tiled=True)


def everywhere(block, axes):
    peers = lax.axis_size(axes)
    return exchange(jnp.broadcast_to(block[None], (peers, *block.shape)), axes)


def from_other_core(block):
    return lax.ppermute(block, "c", [(0, 1), (1, 0)])


def both_cores(block):
    core = lax.axis_index("c")
    other = from_other_core(block)
    first = jnp.where(core == 0, block, other)
    second = jnp.where(core == 0, other, block)
    return jnp.stack([first, second])


def whole_rows(parts):
    c, yx, z, r, n = parts.shape
    parts = parts.reshape(c, 4, 4, z, r, n)
    return parts.transpose(3, 1, 0, 2, 4, 5).reshape(c * yx * z * r, n)


def fill_weights(core, mine_ref, other_ref, whole_ref):
    for z in range(8):
        tiles = []
        for y in range(4):
            mine = [mine_ref[y * 4 + x, z].astype(F32) for x in range(4)]
            other = [other_ref[y * 4 + x, z].astype(F32) for x in range(4)]
            tiles += [jnp.where(core == 0, m, o) for m, o in zip(mine, other)]
            tiles += [jnp.where(core == 0, o, m) for m, o in zip(mine, other)]
        rows = jnp.concatenate(tiles, axis=0).astype(BF)
        whole_ref[pl.ds(z * 256, 256), :] = rows


def terms_to_halves(core, left_ref, right, scale, keep_ref, send_ref):
    for z in range(8):
        left = left_ref[:, pl.ds(z * 256, 256)]
        part = lax.dot_general(left, right, (((0,), (0,)), ((), ())), preferred_element_type=F32)
        part = (part * scale).reshape(4, 2, 4, 8, right.shape[1])
        for y in range(4):
            first, second = part[y, 0], part[y, 1]
            keep_ref[pl.ds(y * 4, 4), z] = jnp.where(core == 0, first, second).astype(BF)
            send_ref[pl.ds(y * 4, 4), z] = jnp.where(core == 0, second, first).astype(BF)


def expand_kernel(scale, core_ref, grad_ref, hidden_ref, keep_ref, send_ref):
    terms_to_halves(core_ref[0], grad_ref, hidden_ref[...], scale, keep_ref, send_ref)


def hidden_kernel(
    inv_m,
    inv_c,
    core_ref,
    saved_ref,
    mine_ref,
    other_ref,
    grad_hbm,
    acts_hbm,
    out_ref,
    keep_ref,
    send_ref,
    whole_ref,
    grad_ref,
    acts_ref,
    sems,
):
    core = core_ref[0]
    grad_copy = pltpu.make_async_copy(grad_hbm, grad_ref, sems.at[0])
    acts_copy = pltpu.make_async_copy(acts_hbm, acts_ref, sems.at[1])
    grad_copy.start()
    acts_copy.start()
    fill_weights(core, mine_ref, other_ref, whole_ref)
    grad_copy.wait()
    summed = jnp.dot(grad_ref[...], whole_ref[...], preferred_element_type=F32)
    saved = saved_ref[...].astype(F32)
    out_ref[...] = jnp.where(saved > 0, summed * inv_m, 0.0).astype(BF)
    acts_copy.wait()
    terms_to_halves(core, acts_ref, out_ref[...], inv_c, keep_ref, send_ref)


def chip_sum_kernel(keep_e_ref, got_e_ref, keep_r_ref, got_r_ref, out_ref):
    for at, (keep_ref, got_ref) in enumerate(((keep_e_ref, got_e_ref), (keep_r_ref, got_r_ref))):
        total = keep_ref[...].astype(F32) + got_ref[...].astype(F32)
        out_ref[:, at] = total.astype(BF)


def chip_sum(*parts):
    peers, *rest = parts[0].shape
    whole = pl.BlockSpec(memory_space=pltpu.VMEM)
    moved = 3 * parts[0].size * 4
    return pl.pallas_call(
        chip_sum_kernel,
        out_shape=jax.ShapeDtypeStruct((peers, 2, *rest), BF),
        in_specs=[whole] * 4,
        out_specs=whole,
        compiler_params=pltpu.CompilerParams(vmem_limit_bytes=16 * 1024 * 1024),
        cost_estimate=pl.CostEstimate(
            flops=2 * parts[0].size, bytes_accessed=moved, transcendentals=0
        ),
    )(*parts)


def back_kernel(inv_c, core_ref, grad_ref, hidden_ref, mine_ref, other_ref, out_ref, whole_ref):
    fill_weights(core_ref[0], mine_ref, other_ref, whole_ref)
    for z in range(8):
        columns = pl.ds(z * 256, 256)
        back = lax.dot_general(
            hidden_ref[...],
            whole_ref[columns, :],
            (((1,), (1,)), ((), ())),
            preferred_element_type=F32,
        )
        out_ref[:, columns] = (grad_ref[:, columns].astype(F32) + back * inv_c).astype(BF)


def local_call(kernel, operands, outs, scratch, flops, streamed=()):
    whole = pl.BlockSpec(memory_space=pltpu.VMEM)
    core = lax.axis_index("c").astype(jnp.int32).reshape(1)
    moved = sum(x.size * x.dtype.itemsize for x in (*operands, *streamed, *outs))
    scratch = scratch + [pltpu.VMEM(x.shape, x.dtype) for x in streamed]
    if streamed:
        scratch = scratch + [pltpu.SemaphoreType.DMA((len(streamed),))]
    return pl.pallas_call(
        kernel,
        out_shape=outs,
        in_specs=[pl.BlockSpec(memory_space=pltpu.SMEM)] + [whole] * len(operands)
        + [pl.BlockSpec(memory_space=pltpu.HBM)] * len(streamed),
        out_specs=[whole] * len(outs),
        scratch_shapes=scratch,
        compiler_params=pltpu.CompilerParams(vmem_limit_bytes=50 * 1024 * 1024),
        cost_estimate=pl.CostEstimate(flops=flops, bytes_accessed=moved, transcendentals=0),
    )(core, *operands, *streamed)


def layer_update(master, grads, velocity, wsquare, gsquare):
    wnorm = jnp.sqrt(wsquare)
    gnorm = jnp.sqrt(gsquare)
    trust = wnorm / (gnorm + 5e-05 * wnorm)
    new_velocity = 0.9 * velocity + trust * (grads + 5e-05 * master)
    new_master = master - 0.1 * new_velocity
    return (new_master, new_velocity)


def step(
    acts, saved_hidden, grad_out, master_reduce, master_expand, velocity_reduce, velocity_expand
):
    channels = grad_out.shape[1]
    middle = saved_hidden.shape[1]
    inv_c = 1.0 / float(channels) ** 0.5
    inv_m = 1.0 / float(middle) ** 0.5
    half = jax.ShapeDtypeStruct((16, 8, channels // 256, middle), BF)
    whole = pltpu.VMEM((channels, middle), BF)
    flops = 2 * grad_out.size * middle

    cur = jnp.stack([master_expand.astype(BF), master_reduce.astype(BF)])
    along_z = everywhere(cur, "z")
    mine = everywhere(along_z[:, 0], ("y", "x"))
    keep_e, send_e = local_call(
        functools.partial(expand_kernel, inv_m), (grad_out, saved_hidden), (half, half), [], flops
    )
    other = from_other_core(mine)
    mine_reduce = everywhere(along_z[:, 1], ("y", "x"))
    grad_hidden, keep_r, send_r = local_call(
        functools.partial(hidden_kernel, inv_m, inv_c),
        (saved_hidden, mine, other),
        (jax.ShapeDtypeStruct(saved_hidden.shape, BF), half, half),
        [whole],
        2 * flops,
        (grad_out, acts),
    )
    halves = chip_sum(keep_e, from_other_core(send_e), keep_r, from_other_core(send_r))
    halves, mine_reduce = lax.optimization_barrier((halves, mine_reduce))
    arrived = exchange(halves, ("y", "x"))
    over_plane = jnp.sum(arrived.astype(F32), axis=0).astype(BF)
    arrived = exchange(over_plane.transpose(1, 0, 2, 3), "z")
    grads = jnp.sum(arrived.astype(F32), axis=0)
    g_expand, g_reduce = grads[0], grads[1]

    other_reduce = from_other_core(mine_reduce)
    (grad_in,) = local_call(
        functools.partial(back_kernel, inv_c),
        (grad_out, grad_hidden, mine_reduce, other_reduce),
        (jax.ShapeDtypeStruct(grad_out.shape, BF),),
        [whole],
        flops,
    )

    squares = jnp.stack(
        [
            jnp.sum(master_expand * master_expand),
            jnp.sum(g_expand * g_expand),
            jnp.sum(master_reduce * master_reduce),
            jnp.sum(g_reduce * g_reduce),
        ]
    )
    squares = everywhere(squares[None], ("z", "y")).sum(axis=0)
    squares = everywhere(squares, ("c", "x")).sum(axis=0)[0]
    new_mr, new_vr = layer_update(master_reduce, g_reduce, velocity_reduce, squares[2], squares[3])
    new_me, new_ve = layer_update(master_expand, g_expand, velocity_expand, squares[0], squares[1])
    work = jnp.stack([new_me.astype(BF), new_mr.astype(BF)])
    along_z = everywhere(work, "z")
    mine = everywhere(along_z, ("y", "x"))
    parts = both_cores(mine)
    work_expand = whole_rows(parts[:, :, :, 0])
    work_reduce = whole_rows(parts[:, :, :, 1])
    return (grad_in, new_mr, new_me, new_vr, new_ve, work_reduce, work_expand)


def solution(mesh):
    finer = Mesh(mesh.devices.reshape(8, 4, 2, 4), ROWS_OVER)
    split = P(ROWS_OVER, None)
    return jax.shard_map(
        step,
        mesh=finer,
        in_specs=(split,) * 7,
        out_specs=(split,) * 5 + (P(), P()),
        check_vma=False,
    )
```

```python
import functools

import jax
import jax.numpy as jnp
from jax import lax
from jax.experimental import pallas as pl
from jax.experimental.pallas import tpu as pltpu
from jax.sharding import Mesh
from jax.sharding import PartitionSpec as P


ROWS_OVER = ("z", "y", "c", "x")
BF = jnp.bfloat16
F32 = jnp.float32


def exchange(parts, axes):
    return lax.all_to_all(parts, axes, 0, 0, tiled=True)


def everywhere(block, axes):
    peers = lax.axis_size(axes)
    return exchange(jnp.broadcast_to(block[None], (peers, *block.shape)), axes)


def from_other_core(block):
    return lax.ppermute(block, "c", [(0, 1), (1, 0)])


def fill_weights(core, mine_ref, other_ref, whole_ref):
    for z in range(8):
        tiles = []
        for y in range(4):
            mine = [mine_ref[y * 4 + x, z].astype(F32) for x in range(4)]
            other = [other_ref[y * 4 + x, z].astype(F32) for x in range(4)]
            tiles += [jnp.where(core == 0, m, o) for m, o in zip(mine, other)]
            tiles += [jnp.where(core == 0, o, m) for m, o in zip(mine, other)]
        rows = jnp.concatenate(tiles, axis=0).astype(BF)
        whole_ref[pl.ds(z * 256, 256), :] = rows


def terms_to_halves(core, left_ref, right, scale, keep_ref, send_ref):
    for z in range(8):
        left = left_ref[:, pl.ds(z * 256, 256)]
        part = lax.dot_general(left, right, (((0,), (0,)), ((), ())), preferred_element_type=F32)
        part = (part * scale).reshape(4, 2, 4, 8, right.shape[1])
        for y in range(4):
            first, second = part[y, 0], part[y, 1]
            keep_ref[pl.ds(y * 4, 4), z] = jnp.where(core == 0, first, second).astype(BF)
            send_ref[pl.ds(y * 4, 4), z] = jnp.where(core == 0, second, first).astype(BF)


def expand_kernel(scale, core_ref, grad_ref, hidden_ref, keep_ref, send_ref):
    terms_to_halves(core_ref[0], grad_ref, hidden_ref[...], scale, keep_ref, send_ref)


def hidden_kernel(
    inv_m,
    inv_c,
    core_ref,
    saved_ref,
    mine_ref,
    other_ref,
    grad_hbm,
    acts_hbm,
    out_ref,
    keep_ref,
    send_ref,
    whole_ref,
    grad_ref,
    acts_ref,
    sems,
):
    core = core_ref[0]
    grad_copy = pltpu.make_async_copy(grad_hbm, grad_ref, sems.at[0])
    acts_copy = pltpu.make_async_copy(acts_hbm, acts_ref, sems.at[1])
    grad_copy.start()
    acts_copy.start()
    fill_weights(core, mine_ref, other_ref, whole_ref)
    grad_copy.wait()
    summed = jnp.dot(grad_ref[...], whole_ref[...], preferred_element_type=F32)
    saved = saved_ref[...].astype(F32)
    out_ref[...] = jnp.where(saved > 0, summed * inv_m, 0.0).astype(BF)
    acts_copy.wait()
    terms_to_halves(core, acts_ref, out_ref[...], inv_c, keep_ref, send_ref)


def chip_sum_kernel(keep_e_ref, got_e_ref, keep_r_ref, got_r_ref, out_ref):
    for at, (keep_ref, got_ref) in enumerate(((keep_e_ref, got_e_ref), (keep_r_ref, got_r_ref))):
        total = keep_ref[...].astype(F32) + got_ref[...].astype(F32)
        out_ref[:, at] = total.astype(BF)


def chip_sum(*parts):
    peers, *rest = parts[0].shape
    whole = pl.BlockSpec(memory_space=pltpu.VMEM)
    moved = 3 * parts[0].size * 4
    return pl.pallas_call(
        chip_sum_kernel,
        out_shape=jax.ShapeDtypeStruct((peers, 2, *rest), BF),
        in_specs=[whole] * 4,
        out_specs=whole,
        compiler_params=pltpu.CompilerParams(vmem_limit_bytes=16 * 1024 * 1024),
        cost_estimate=pl.CostEstimate(
            flops=2 * parts[0].size, bytes_accessed=moved, transcendentals=0
        ),
    )(*parts)


def back_kernel(inv_c, core_ref, grad_ref, hidden_ref, mine_ref, other_ref, out_ref, whole_ref):
    fill_weights(core_ref[0], mine_ref, other_ref, whole_ref)
    for z in range(8):
        columns = pl.ds(z * 256, 256)
        back = lax.dot_general(
            hidden_ref[...],
            whole_ref[columns, :],
            (((1,), (1,)), ((), ())),
            preferred_element_type=F32,
        )
        out_ref[:, columns] = (grad_ref[:, columns].astype(F32) + back * inv_c).astype(BF)


def local_call(kernel, operands, outs, scratch, flops, streamed=()):
    whole = pl.BlockSpec(memory_space=pltpu.VMEM)
    core = lax.axis_index("c").astype(jnp.int32).reshape(1)
    moved = sum(x.size * x.dtype.itemsize for x in (*operands, *streamed, *outs))
    scratch = scratch + [pltpu.VMEM(x.shape, x.dtype) for x in streamed]
    if streamed:
        scratch = scratch + [pltpu.SemaphoreType.DMA((len(streamed),))]
    return pl.pallas_call(
        kernel,
        out_shape=outs,
        in_specs=[pl.BlockSpec(memory_space=pltpu.SMEM)] + [whole] * len(operands)
        + [pl.BlockSpec(memory_space=pltpu.HBM)] * len(streamed),
        out_specs=[whole] * len(outs),
        scratch_shapes=scratch,
        compiler_params=pltpu.CompilerParams(vmem_limit_bytes=50 * 1024 * 1024),
        cost_estimate=pl.CostEstimate(flops=flops, bytes_accessed=moved, transcendentals=0),
    )(core, *operands, *streamed)


def total_of(terms):
    return jnp.sum(jnp.sum(terms, axis=1, keepdims=True), axis=0, keepdims=True)


def owner_kernel(arrived_ref, me_ref, mr_ref, ve_ref, vr_ref, grads_ref, out_ref):
    tiles, squares = [], []
    moved = []
    for layer, (m_ref, v_ref) in enumerate(((me_ref, ve_ref), (mr_ref, vr_ref))):
        grads = arrived_ref[0, layer].astype(F32)
        for z in range(1, 8):
            grads = grads + arrived_ref[z, layer].astype(F32)
        grads_ref[layer] = grads
        master = m_ref[...]
        tiles.append((grads + 5e-05 * master).astype(BF))
        moved.append((master - 0.1 * (0.9 * v_ref[...])).astype(BF))
        squares += [total_of(master * master), total_of(grads * grads)]
    tiles += moved
    rows = lax.broadcasted_iota(jnp.int32, (8, 128), 0)
    left = jnp.zeros((8, 128), F32)
    for at, square in enumerate(squares):
        left = jnp.where(rows == at, square, left)
    parts = []
    for _ in range(3):
        part = left.astype(BF)
        left = left - part.astype(F32)
        parts.append(part)
    tiles.append(jnp.concatenate(parts + [jnp.zeros((8, 128), BF)], axis=1))
    for z in range(8):
        for at, tile in enumerate(tiles):
            out_ref[z, at] = tile


def ring_squares_kernel(ring_ref, out_ref):
    total = jnp.zeros((8, 128), F32)
    for z in range(8):
        packed = ring_ref[z, 4].astype(F32)
        total = total + ((packed[:, :128] + packed[:, 128:256]) + packed[:, 256:384])
    out_ref[...] = jnp.broadcast_to(total[None], out_ref.shape)


def update_kernel(
    squares_ref,
    ring_ref,
    grads_ref,
    me_ref,
    mr_ref,
    ve_ref,
    vr_ref,
    new_me_ref,
    new_mr_ref,
    new_ve_ref,
    new_vr_ref,
    work_ref,
):
    squares = squares_ref[0]
    for peer in range(1, squares_ref.shape[0]):
        squares = squares + squares_ref[peer]
    norms = jnp.sqrt(squares)
    layers = (
        (me_ref, ve_ref, new_me_ref, new_ve_ref),
        (mr_ref, vr_ref, new_mr_ref, new_vr_ref),
    )
    for layer, (m_ref, v_ref, new_m_ref, new_v_ref) in enumerate(layers):
        wnorm = norms[2 * layer : 2 * layer + 1, :1]
        gnorm = norms[2 * layer + 1 : 2 * layer + 2, :1]
        trust = wnorm / (gnorm + 5e-05 * wnorm)
        master = m_ref[...]
        new_velocity = 0.9 * v_ref[...] + trust * (grads_ref[layer] + 5e-05 * master)
        new_v_ref[...] = new_velocity
        new_m_ref[...] = master - 0.1 * new_velocity
        for z in range(8):
            step = 0.1 * (trust * ring_ref[z, layer].astype(F32))
            work_ref[z, layer] = (ring_ref[z, 2 + layer].astype(F32) - step).astype(BF)


def small_call(kernel, operands, outs):
    whole = pl.BlockSpec(memory_space=pltpu.VMEM)
    moved = sum(x.size * x.dtype.itemsize for x in (*operands, *outs))
    return pl.pallas_call(
        kernel,
        out_shape=outs,
        in_specs=[whole] * len(operands),
        out_specs=[whole] * len(outs),
        compiler_params=pltpu.CompilerParams(vmem_limit_bytes=16 * 1024 * 1024),
        cost_estimate=pl.CostEstimate(flops=moved, bytes_accessed=moved, transcendentals=0),
    )(*operands)


def place_kernel(core_ref, parts_ref, *refs):
    expand_ref, reduce_ref, sems = refs[-3:]
    core = core_ref[0]
    copies = []
    for y in range(4):
        for x in range(4):
            for layer, out_ref in enumerate((expand_ref, reduce_ref)):
                copies.append(
                    pltpu.make_async_copy(
                        parts_ref.at[y * 4 + x, :, layer],
                        out_ref.at[:, y, core, x],
                        sems.at[len(copies)],
                    )
                )
    for copy in copies:
        copy.start()
    for copy in copies:
        copy.wait()


def place(core, parts, into):
    _, z, _, r, n = parts.shape
    whole = jax.ShapeDtypeStruct((z, 4, 2, 4, r, n), BF)
    hbm = pl.BlockSpec(memory_space=pl.ANY)
    return pl.pallas_call(
        place_kernel,
        out_shape=(whole, whole),
        in_specs=[
            pl.BlockSpec(memory_space=pltpu.SMEM),
            pl.BlockSpec(memory_space=pltpu.VMEM),
        ]
        + [hbm] * len(into),
        out_specs=(hbm, hbm),
        scratch_shapes=[pltpu.SemaphoreType.DMA((32,))],
        input_output_aliases={2 + at: at for at in range(len(into))},
        compiler_params=pltpu.CompilerParams(vmem_limit_bytes=8 * 1024 * 1024),
        cost_estimate=pl.CostEstimate(
            flops=parts.size, bytes_accessed=4 * parts.size, transcendentals=0
        ),
    )(core.astype(jnp.int32).reshape(1), parts, *into)


def step(
    acts, saved_hidden, grad_out, master_reduce, master_expand, velocity_reduce, velocity_expand
):
    channels = grad_out.shape[1]
    middle = saved_hidden.shape[1]
    inv_c = 1.0 / float(channels) ** 0.5
    inv_m = 1.0 / float(middle) ** 0.5
    half = jax.ShapeDtypeStruct((16, 8, channels // 256, middle), BF)
    whole = pltpu.VMEM((channels, middle), BF)
    flops = 2 * grad_out.size * middle

    cur = jnp.stack([master_expand.astype(BF), master_reduce.astype(BF)])
    along_z = everywhere(cur, "z")
    mine = everywhere(along_z[:, 0], ("y", "x"))
    keep_e, send_e = local_call(
        functools.partial(expand_kernel, inv_m), (grad_out, saved_hidden), (half, half), [], flops
    )
    other = from_other_core(mine)
    mine_reduce = everywhere(along_z[:, 1], ("y", "x"))
    grad_hidden, keep_r, send_r = local_call(
        functools.partial(hidden_kernel, inv_m, inv_c),
        (saved_hidden, mine, other),
        (jax.ShapeDtypeStruct(saved_hidden.shape, BF), half, half),
        [whole],
        2 * flops,
        (grad_out, acts),
    )
    halves = chip_sum(keep_e, from_other_core(send_e), keep_r, from_other_core(send_r))
    halves, mine_reduce = lax.optimization_barrier((halves, mine_reduce))
    arrived = exchange(halves, ("y", "x"))
    over_plane = jnp.sum(arrived.astype(F32), axis=0).astype(BF)
    arrived = exchange(over_plane.transpose(1, 0, 2, 3), "z")
    other_reduce = from_other_core(mine_reduce)
    (grad_in,) = local_call(
        functools.partial(back_kernel, inv_c),
        (grad_out, grad_hidden, mine_reduce, other_reduce),
        (jax.ShapeDtypeStruct(grad_out.shape, BF),),
        [whole],
        flops,
    )

    state = (master_expand, master_reduce, velocity_expand, velocity_reduce)
    own = jax.ShapeDtypeStruct(master_expand.shape, F32)
    grads, rows = small_call(
        owner_kernel,
        (arrived, *state),
        (
            jax.ShapeDtypeStruct((2, *own.shape), F32),
            jax.ShapeDtypeStruct((8, 5, *own.shape), BF),
        ),
    )
    ring = exchange(rows, "z")
    (squares,) = small_call(
        ring_squares_kernel, (ring,), (jax.ShapeDtypeStruct((32, 8, 128), F32),)
    )
    squares = exchange(squares, ("y", "c", "x"))
    new_me, new_mr, new_ve, new_vr, work = small_call(
        update_kernel,
        (squares, ring, grads, *state),
        (own, own, own, own, jax.ShapeDtypeStruct((8, 2, *own.shape), BF)),
    )
    mine = everywhere(work, ("y", "x"))
    core = lax.axis_index("c")
    other = from_other_core(mine)
    placed = place(core, mine, ())
    placed = place(1 - core, other, placed)
    work_expand, work_reduce = (p.reshape(channels, middle) for p in placed)
    return (grad_in, new_mr, new_me, new_vr, new_ve, work_reduce, work_expand)


def solution(mesh):
    finer = Mesh(mesh.devices.reshape(8, 4, 2, 4), ROWS_OVER)
    split = P(ROWS_OVER, None)
    return jax.shard_map(
        step,
        mesh=finer,
        in_specs=(split,) * 7,
        out_specs=(split,) * 5 + (P(), P()),
        check_vma=False,
    )
```

```python
import functools

import jax
import jax.numpy as jnp
from jax import lax
from jax.experimental import pallas as pl
from jax.experimental.pallas import tpu as pltpu
from jax.sharding import Mesh
from jax.sharding import PartitionSpec as P


ROWS_OVER = ("z", "y", "c", "x")
BF = jnp.bfloat16
F32 = jnp.float32


def exchange(parts, axes):
    return lax.all_to_all(parts, axes, 0, 0, tiled=True)


def everywhere(block, axes):
    peers = lax.axis_size(axes)
    return exchange(jnp.broadcast_to(block[None], (peers, *block.shape)), axes)


def shifted(block, axis):
    pieces = [block]
    for s in range(1, 4):
        pieces.append(lax.ppermute(block, axis, [(i, (i + s) % 4) for i in range(4)]))
    return jnp.stack(pieces)


def from_other_core(block):
    return lax.ppermute(block, "c", [(0, 1), (1, 0)])


def fill_weights(core, piece, mine_ref, other_ref, whole_ref):
    for z in range(8):
        tiles = []
        for y in range(4):
            at = [piece(y, x) for x in range(4)]
            mine = [mine_ref[i, z].astype(F32) for i in at]
            other = [other_ref[i, z].astype(F32) for i in at]
            tiles += [jnp.where(core == 0, m, o) for m, o in zip(mine, other)]
            tiles += [jnp.where(core == 0, o, m) for m, o in zip(mine, other)]
        rows = jnp.concatenate(tiles, axis=0).astype(BF)
        whole_ref[pl.ds(z * 256, 256), :] = rows


def terms_to_halves(core, left_ref, right, scale, keep_ref, send_ref):
    for z in range(8):
        left = left_ref[:, pl.ds(z * 256, 256)]
        part = lax.dot_general(left, right, (((0,), (0,)), ((), ())), preferred_element_type=F32)
        part = (part * scale).reshape(4, 2, 4, 8, right.shape[1])
        for y in range(4):
            first, second = part[y, 0], part[y, 1]
            keep_ref[pl.ds(y * 4, 4), z] = jnp.where(core == 0, first, second).astype(BF)
            send_ref[pl.ds(y * 4, 4), z] = jnp.where(core == 0, second, first).astype(BF)


def expand_kernel(scale, place_ref, grad_ref, hidden_ref, keep_ref, send_ref):
    terms_to_halves(place_ref[0], grad_ref, hidden_ref[...], scale, keep_ref, send_ref)


def hidden_kernel(
    inv_m,
    inv_c,
    place_ref,
    saved_ref,
    mine_ref,
    other_ref,
    grad_hbm,
    acts_hbm,
    out_ref,
    keep_ref,
    send_ref,
    whole_ref,
    grad_ref,
    acts_ref,
    sems,
):
    core = place_ref[0]
    grad_copy = pltpu.make_async_copy(grad_hbm, grad_ref, sems.at[0])
    acts_copy = pltpu.make_async_copy(acts_hbm, acts_ref, sems.at[1])
    grad_copy.start()
    acts_copy.start()
    fill_weights(core, lambda y, x: y * 4 + x, mine_ref, other_ref, whole_ref)
    grad_copy.wait()
    summed = jnp.dot(grad_ref[...], whole_ref[...], preferred_element_type=F32)
    saved = saved_ref[...].astype(F32)
    out_ref[...] = jnp.where(saved > 0, summed * inv_m, 0.0).astype(BF)
    acts_copy.wait()
    terms_to_halves(core, acts_ref, out_ref[...], inv_c, keep_ref, send_ref)


def chip_sum_kernel(keep_ref, got_ref, out_ref):
    out_ref[...] = (keep_ref[...].astype(F32) + got_ref[...].astype(F32)).astype(BF)


def plane_sum_kernel(expand_ref, reduce_ref, out_ref):
    for z in range(8):
        out_ref[z, 0] = expand_ref[z]
        total = reduce_ref[0, z].astype(F32)
        for peer in range(1, reduce_ref.shape[0]):
            total = total + reduce_ref[peer, z].astype(F32)
        out_ref[z, 1] = total.astype(BF)


def back_kernel(inv_c, place_ref, grad_ref, hidden_ref, mine_ref, other_ref, out_ref, whole_ref):
    core, my_y, my_x = place_ref[0], place_ref[1], place_ref[2]

    def piece(y, x):
        return lax.rem(my_y - y + 4, 4) * 4 + lax.rem(my_x - x + 4, 4)

    fill_weights(core, piece, mine_ref, other_ref, whole_ref)
    for z in range(8):
        columns = pl.ds(z * 256, 256)
        back = lax.dot_general(
            hidden_ref[...],
            whole_ref[columns, :],
            (((1,), (1,)), ((), ())),
            preferred_element_type=F32,
        )
        out_ref[:, columns] = (grad_ref[:, columns].astype(F32) + back * inv_c).astype(BF)


def local_call(kernel, operands, outs, scratch, flops, streamed=()):
    whole = pl.BlockSpec(memory_space=pltpu.VMEM)
    at = jnp.stack([lax.axis_index(axis).astype(jnp.int32) for axis in ("c", "y", "x")])
    moved = sum(x.size * x.dtype.itemsize for x in (*operands, *streamed, *outs))
    scratch = scratch + [pltpu.VMEM(x.shape, x.dtype) for x in streamed]
    if streamed:
        scratch = scratch + [pltpu.SemaphoreType.DMA((len(streamed),))]
    return pl.pallas_call(
        kernel,
        out_shape=outs,
        in_specs=[pl.BlockSpec(memory_space=pltpu.SMEM)] + [whole] * len(operands)
        + [pl.BlockSpec(memory_space=pltpu.HBM)] * len(streamed),
        out_specs=[whole] * len(outs),
        scratch_shapes=scratch,
        compiler_params=pltpu.CompilerParams(vmem_limit_bytes=50 * 1024 * 1024),
        cost_estimate=pl.CostEstimate(flops=flops, bytes_accessed=moved, transcendentals=0),
    )(at, *operands, *streamed)


def total_of(terms):
    return jnp.sum(jnp.sum(terms, axis=1, keepdims=True), axis=0, keepdims=True)


def owner_kernel(arrived_ref, me_ref, mr_ref, ve_ref, vr_ref, grads_ref, out_ref):
    tiles, squares = [], []
    moved = []
    for layer, (m_ref, v_ref) in enumerate(((me_ref, ve_ref), (mr_ref, vr_ref))):
        grads = arrived_ref[0, layer].astype(F32)
        for z in range(1, 8):
            grads = grads + arrived_ref[z, layer].astype(F32)
        grads_ref[layer] = grads
        master = m_ref[...]
        tiles.append((grads + 5e-05 * master).astype(BF))
        moved.append((master - 0.1 * (0.9 * v_ref[...])).astype(BF))
        squares += [total_of(master * master), total_of(grads * grads)]
    tiles += moved
    rows = lax.broadcasted_iota(jnp.int32, (8, 128), 0)
    left = jnp.zeros((8, 128), F32)
    for at, square in enumerate(squares):
        left = jnp.where(rows == at, square, left)
    parts = []
    for _ in range(3):
        part = left.astype(BF)
        left = left - part.astype(F32)
        parts.append(part)
    tiles.append(jnp.concatenate(parts + [jnp.zeros((8, 128), BF)], axis=1))
    for z in range(8):
        for at, tile in enumerate(tiles):
            out_ref[z, at] = tile


def ring_squares_kernel(ring_ref, out_ref):
    total = jnp.zeros((8, 128), F32)
    for z in range(8):
        packed = ring_ref[z, 4].astype(F32)
        total = total + ((packed[:, :128] + packed[:, 128:256]) + packed[:, 256:384])
    out_ref[...] = jnp.broadcast_to(total[None], out_ref.shape)


def update_kernel(
    squares_ref,
    ring_ref,
    grads_ref,
    me_ref,
    mr_ref,
    ve_ref,
    vr_ref,
    new_me_ref,
    new_mr_ref,
    new_ve_ref,
    new_vr_ref,
    work_ref,
):
    squares = squares_ref[0]
    for peer in range(1, squares_ref.shape[0]):
        squares = squares + squares_ref[peer]
    norms = jnp.sqrt(squares)
    layers = (
        (me_ref, ve_ref, new_me_ref, new_ve_ref),
        (mr_ref, vr_ref, new_mr_ref, new_vr_ref),
    )
    for layer, (m_ref, v_ref, new_m_ref, new_v_ref) in enumerate(layers):
        wnorm = norms[2 * layer : 2 * layer + 1, :1]
        gnorm = norms[2 * layer + 1 : 2 * layer + 2, :1]
        trust = wnorm / (gnorm + 5e-05 * wnorm)
        master = m_ref[...]
        new_velocity = 0.9 * v_ref[...] + trust * (grads_ref[layer] + 5e-05 * master)
        new_v_ref[...] = new_velocity
        new_m_ref[...] = master - 0.1 * new_velocity
        for z in range(8):
            step = 0.1 * (trust * ring_ref[z, layer].astype(F32))
            work_ref[z, layer] = (ring_ref[z, 2 + layer].astype(F32) - step).astype(BF)


def small_call(kernel, operands, outs):
    whole = pl.BlockSpec(memory_space=pltpu.VMEM)
    moved = sum(x.size * x.dtype.itemsize for x in (*operands, *outs))
    return pl.pallas_call(
        kernel,
        out_shape=outs,
        in_specs=[whole] * len(operands),
        out_specs=[whole] * len(outs),
        compiler_params=pltpu.CompilerParams(vmem_limit_bytes=16 * 1024 * 1024),
        cost_estimate=pl.CostEstimate(flops=moved, bytes_accessed=moved, transcendentals=0),
    )(*operands)


def place_kernel(core_ref, parts_ref, *refs):
    expand_ref, reduce_ref, sems = refs[-3:]
    core = core_ref[0]
    copies = []
    for y in range(4):
        for x in range(4):
            for layer, out_ref in enumerate((expand_ref, reduce_ref)):
                copies.append(
                    pltpu.make_async_copy(
                        parts_ref.at[y * 4 + x, :, layer],
                        out_ref.at[:, y, core, x],
                        sems.at[len(copies)],
                    )
                )
    for copy in copies:
        copy.start()
    for copy in copies:
        copy.wait()


def place(core, parts, into):
    _, z, _, r, n = parts.shape
    whole = jax.ShapeDtypeStruct((z, 4, 2, 4, r, n), BF)
    hbm = pl.BlockSpec(memory_space=pl.ANY)
    return pl.pallas_call(
        place_kernel,
        out_shape=(whole, whole),
        in_specs=[
            pl.BlockSpec(memory_space=pltpu.SMEM),
            pl.BlockSpec(memory_space=pltpu.VMEM),
        ]
        + [hbm] * len(into),
        out_specs=(hbm, hbm),
        scratch_shapes=[pltpu.SemaphoreType.DMA((32,))],
        input_output_aliases={2 + at: at for at in range(len(into))},
        compiler_params=pltpu.CompilerParams(vmem_limit_bytes=8 * 1024 * 1024),
        cost_estimate=pl.CostEstimate(
            flops=parts.size, bytes_accessed=4 * parts.size, transcendentals=0
        ),
    )(core.astype(jnp.int32).reshape(1), parts, *into)


def step(
    acts, saved_hidden, grad_out, master_reduce, master_expand, velocity_reduce, velocity_expand
):
    channels = grad_out.shape[1]
    middle = saved_hidden.shape[1]
    inv_c = 1.0 / float(channels) ** 0.5
    inv_m = 1.0 / float(middle) ** 0.5
    half = jax.ShapeDtypeStruct((16, 8, channels // 256, middle), BF)
    whole = pltpu.VMEM((channels, middle), BF)
    flops = 2 * grad_out.size * middle

    cur = jnp.stack([master_expand.astype(BF), master_reduce.astype(BF)])
    along_z = everywhere(cur, "z")
    mine = everywhere(along_z[:, 0], ("y", "x"))
    keep_e, send_e = local_call(
        functools.partial(expand_kernel, inv_m), (grad_out, saved_hidden), (half, half), [], flops
    )
    (sent_e,) = small_call(chip_sum_kernel, (keep_e, from_other_core(send_e)), (half,))
    other = from_other_core(mine)
    arrived_e = exchange(sent_e, ("y", "x"))
    grad_hidden, keep_r, send_r = local_call(
        functools.partial(hidden_kernel, inv_m, inv_c),
        (saved_hidden, mine, other),
        (jax.ShapeDtypeStruct(saved_hidden.shape, BF), half, half),
        [whole],
        2 * flops,
        (grad_out, acts),
    )
    (sent_r,) = small_call(chip_sum_kernel, (keep_r, from_other_core(send_r)), (half,))
    arrived_r = exchange(sent_r, ("y", "x"))
    row = shifted(along_z[:, 1], "x")
    plane_e = jnp.sum(arrived_e.astype(F32), axis=0).astype(BF)
    (over_plane,) = small_call(
        plane_sum_kernel,
        (plane_e, arrived_r),
        (jax.ShapeDtypeStruct((8, 2, channels // 256, middle), BF),),
    )
    arrived = exchange(over_plane, "z")
    mine_reduce = shifted(row, "y").reshape(half.shape)
    other_reduce = from_other_core(mine_reduce)
    (grad_in,) = local_call(
        functools.partial(back_kernel, inv_c),
        (grad_out, grad_hidden, mine_reduce, other_reduce),
        (jax.ShapeDtypeStruct(grad_out.shape, BF),),
        [whole],
        flops,
    )

    state = (master_expand, master_reduce, velocity_expand, velocity_reduce)
    own = jax.ShapeDtypeStruct(master_expand.shape, F32)
    grads, rows = small_call(
        owner_kernel,
        (arrived, *state),
        (
            jax.ShapeDtypeStruct((2, *own.shape), F32),
            jax.ShapeDtypeStruct((8, 5, *own.shape), BF),
        ),
    )
    ring = exchange(rows, "z")
    (squares,) = small_call(
        ring_squares_kernel, (ring,), (jax.ShapeDtypeStruct((32, 8, 128), F32),)
    )
    squares = exchange(squares, ("y", "c", "x"))
    new_me, new_mr, new_ve, new_vr, work = small_call(
        update_kernel,
        (squares, ring, grads, *state),
        (own, own, own, own, jax.ShapeDtypeStruct((8, 2, *own.shape), BF)),
    )
    mine = everywhere(work, ("y", "x"))
    core = lax.axis_index("c")
    other = from_other_core(mine)
    placed = place(core, mine, ())
    placed = place(1 - core, other, placed)
    work_expand, work_reduce = (p.reshape(channels, middle) for p in placed)
    return (grad_in, new_mr, new_me, new_vr, new_ve, work_reduce, work_expand)


def solution(mesh):
    finer = Mesh(mesh.devices.reshape(8, 4, 2, 4), ROWS_OVER)
    split = P(ROWS_OVER, None)
    return jax.shard_map(
        step,
        mesh=finer,
        in_specs=(split,) * 7,
        out_specs=(split,) * 5 + (P(), P()),
        check_vma=False,
    )
```

```python
import functools

import jax
import jax.numpy as jnp
from jax import lax
from jax.experimental import pallas as pl
from jax.experimental.pallas import tpu as pltpu
from jax.sharding import Mesh
from jax.sharding import PartitionSpec as P


ROWS_OVER = ("z", "y", "c", "x")
BF = jnp.bfloat16
F32 = jnp.float32


def exchange(parts, axes):
    return lax.all_to_all(parts, axes, 0, 0, tiled=True)


def everywhere(block, axes):
    peers = lax.axis_size(axes)
    return exchange(jnp.broadcast_to(block[None], (peers, *block.shape)), axes)


def shifted(block, axis):
    pieces = [block]
    for s in range(1, 4):
        pieces.append(lax.ppermute(block, axis, [(i, (i + s) % 4) for i in range(4)]))
    return jnp.concatenate(pieces)


def from_other_core(block):
    return lax.ppermute(block, "c", [(0, 1), (1, 0)])


def fill_weights(core, piece, mine_ref, other_ref, whole_ref):
    for z in range(8):
        tiles = []
        for y in range(4):
            at = [piece(y, x) for x in range(4)]
            mine = [mine_ref[i, z].astype(F32) for i in at]
            other = [other_ref[i, z].astype(F32) for i in at]
            tiles += [jnp.where(core == 0, m, o) for m, o in zip(mine, other)]
            tiles += [jnp.where(core == 0, o, m) for m, o in zip(mine, other)]
        rows = jnp.concatenate(tiles, axis=0).astype(BF)
        whole_ref[pl.ds(z * 256, 256), :] = rows


def terms_to_halves(core, left_ref, right, scale, keep_ref, send_ref):
    for z in range(8):
        left = left_ref[:, pl.ds(z * 256, 256)]
        part = lax.dot_general(left, right, (((0,), (0,)), ((), ())), preferred_element_type=F32)
        part = (part * scale).reshape(4, 2, 4, 8, right.shape[1])
        for y in range(4):
            first, second = part[y, 0], part[y, 1]
            keep_ref[pl.ds(y * 4, 4), z] = jnp.where(core == 0, first, second).astype(BF)
            send_ref[pl.ds(y * 4, 4), z] = jnp.where(core == 0, second, first).astype(BF)


def expand_kernel(scale, place_ref, grad_ref, hidden_ref, keep_ref, send_ref):
    terms_to_halves(place_ref[0], grad_ref, hidden_ref[...], scale, keep_ref, send_ref)


def hidden_kernel(
    inv_m,
    inv_c,
    place_ref,
    saved_ref,
    mine_ref,
    other_ref,
    grad_hbm,
    acts_hbm,
    out_ref,
    keep_ref,
    send_ref,
    whole_ref,
    grad_ref,
    acts_ref,
    sems,
):
    core = place_ref[0]
    grad_copy = pltpu.make_async_copy(grad_hbm, grad_ref, sems.at[0])
    acts_copy = pltpu.make_async_copy(acts_hbm, acts_ref, sems.at[1])
    grad_copy.start()
    acts_copy.start()
    fill_weights(core, lambda y, x: y * 4 + x, mine_ref, other_ref, whole_ref)
    grad_copy.wait()
    summed = jnp.dot(grad_ref[...], whole_ref[...], preferred_element_type=F32)
    saved = saved_ref[...].astype(F32)
    out_ref[...] = jnp.where(saved > 0, summed * inv_m, 0.0).astype(BF)
    acts_copy.wait()
    terms_to_halves(core, acts_ref, out_ref[...], inv_c, keep_ref, send_ref)


def working_kernel(me_ref, mr_ref, out_ref):
    for layer, m_ref in enumerate((me_ref, mr_ref)):
        rows = m_ref[...].astype(BF)
        for z in range(8):
            out_ref[z, layer] = rows


def chip_sum_kernel(keep_ref, got_ref, out_ref):
    out_ref[...] = (keep_ref[...].astype(F32) + got_ref[...].astype(F32)).astype(BF)


def plane_sum_kernel(expand_ref, reduce_ref, out_ref):
    for z in range(8):
        out_ref[z, 0] = expand_ref[z]
        total = reduce_ref[0, z].astype(F32)
        for peer in range(1, reduce_ref.shape[0]):
            total = total + reduce_ref[peer, z].astype(F32)
        out_ref[z, 1] = total.astype(BF)


def back_kernel(inv_c, place_ref, grad_ref, hidden_ref, mine_ref, other_ref, out_ref, whole_ref):
    core, my_y, my_x = place_ref[0], place_ref[1], place_ref[2]

    def piece(y, x):
        return lax.rem(my_y - y + 4, 4) * 4 + lax.rem(my_x - x + 4, 4)

    fill_weights(core, piece, mine_ref, other_ref, whole_ref)
    for z in range(8):
        columns = pl.ds(z * 256, 256)
        back = lax.dot_general(
            hidden_ref[...],
            whole_ref[columns, :],
            (((1,), (1,)), ((), ())),
            preferred_element_type=F32,
        )
        out_ref[:, columns] = (grad_ref[:, columns].astype(F32) + back * inv_c).astype(BF)


def local_call(kernel, operands, outs, scratch, flops, streamed=()):
    whole = pl.BlockSpec(memory_space=pltpu.VMEM)
    at = jnp.stack([lax.axis_index(axis).astype(jnp.int32) for axis in ("c", "y", "x")])
    moved = sum(x.size * x.dtype.itemsize for x in (*operands, *streamed, *outs))
    scratch = scratch + [pltpu.VMEM(x.shape, x.dtype) for x in streamed]
    if streamed:
        scratch = scratch + [pltpu.SemaphoreType.DMA((len(streamed),))]
    return pl.pallas_call(
        kernel,
        out_shape=outs,
        in_specs=[pl.BlockSpec(memory_space=pltpu.SMEM)] + [whole] * len(operands)
        + [pl.BlockSpec(memory_space=pltpu.HBM)] * len(streamed),
        out_specs=[whole] * len(outs),
        scratch_shapes=scratch,
        compiler_params=pltpu.CompilerParams(vmem_limit_bytes=50 * 1024 * 1024),
        cost_estimate=pl.CostEstimate(flops=flops, bytes_accessed=moved, transcendentals=0),
    )(at, *operands, *streamed)


def total_of(terms):
    return jnp.sum(jnp.sum(terms, axis=1, keepdims=True), axis=0, keepdims=True)


def owner_kernel(arrived_ref, me_ref, mr_ref, ve_ref, vr_ref, grads_ref, out_ref):
    tiles, squares = [], []
    moved = []
    for layer, (m_ref, v_ref) in enumerate(((me_ref, ve_ref), (mr_ref, vr_ref))):
        grads = arrived_ref[0, layer].astype(F32)
        for z in range(1, 8):
            grads = grads + arrived_ref[z, layer].astype(F32)
        grads_ref[layer] = grads
        master = m_ref[...]
        tiles.append((grads + 5e-05 * master).astype(BF))
        moved.append((master - 0.1 * (0.9 * v_ref[...])).astype(BF))
        squares += [total_of(master * master), total_of(grads * grads)]
    tiles += moved
    rows = lax.broadcasted_iota(jnp.int32, (8, 128), 0)
    left = jnp.zeros((8, 128), F32)
    for at, square in enumerate(squares):
        left = jnp.where(rows == at, square, left)
    parts = []
    for _ in range(3):
        part = left.astype(BF)
        left = left - part.astype(F32)
        parts.append(part)
    tiles.append(jnp.concatenate(parts + [jnp.zeros((8, 128), BF)], axis=1))
    for z in range(8):
        for at, tile in enumerate(tiles):
            out_ref[z, at] = tile


def ring_squares_kernel(ring_ref, out_ref):
    total = jnp.zeros((8, 128), F32)
    for z in range(8):
        packed = ring_ref[z, 4].astype(F32)
        total = total + ((packed[:, :128] + packed[:, 128:256]) + packed[:, 256:384])
    out_ref[...] = jnp.broadcast_to(total[None], out_ref.shape)


def update_kernel(
    squares_ref,
    ring_ref,
    grads_ref,
    me_ref,
    mr_ref,
    ve_ref,
    vr_ref,
    new_me_ref,
    new_mr_ref,
    new_ve_ref,
    new_vr_ref,
    work_ref,
):
    squares = squares_ref[0]
    for peer in range(1, squares_ref.shape[0]):
        squares = squares + squares_ref[peer]
    norms = jnp.sqrt(squares)
    layers = (
        (me_ref, ve_ref, new_me_ref, new_ve_ref),
        (mr_ref, vr_ref, new_mr_ref, new_vr_ref),
    )
    for layer, (m_ref, v_ref, new_m_ref, new_v_ref) in enumerate(layers):
        wnorm = norms[2 * layer : 2 * layer + 1, :1]
        gnorm = norms[2 * layer + 1 : 2 * layer + 2, :1]
        trust = wnorm / (gnorm + 5e-05 * wnorm)
        master = m_ref[...]
        new_velocity = 0.9 * v_ref[...] + trust * (grads_ref[layer] + 5e-05 * master)
        new_v_ref[...] = new_velocity
        new_m_ref[...] = master - 0.1 * new_velocity
        for z in range(8):
            step = 0.1 * (trust * ring_ref[z, layer].astype(F32))
            work_ref[z, layer] = (ring_ref[z, 2 + layer].astype(F32) - step).astype(BF)


def small_call(kernel, operands, outs):
    whole = pl.BlockSpec(memory_space=pltpu.VMEM)
    moved = sum(x.size * x.dtype.itemsize for x in (*operands, *outs))
    return pl.pallas_call(
        kernel,
        out_shape=outs,
        in_specs=[whole] * len(operands),
        out_specs=[whole] * len(outs),
        compiler_params=pltpu.CompilerParams(vmem_limit_bytes=16 * 1024 * 1024),
        cost_estimate=pl.CostEstimate(flops=moved, bytes_accessed=moved, transcendentals=0),
    )(*operands)


def placements(core, y, parts_ref, out_refs, sems):
    copies = []
    for x in range(4):
        for layer, out_ref in enumerate(out_refs):
            copies.append(
                pltpu.make_async_copy(
                    parts_ref.at[y * 4 + x, :, layer],
                    out_ref.at[:, y, core, x],
                    sems.at[y * 8 + x * 2 + layer],
                )
            )
    return copies


def place_mine_kernel(core_ref, parts_ref, expand_ref, reduce_ref, sems):
    copies = []
    for y in range(4):
        copies += placements(core_ref[0], y, parts_ref, (expand_ref, reduce_ref), sems)
    for copy in copies:
        copy.start()
    for copy in copies:
        copy.wait()


def place_other_kernel(
    core_ref, parts_hbm, _expand, _reduce, expand_ref, reduce_ref, parts_ref, sems, in_sems
):
    loads = [
        pltpu.make_async_copy(
            parts_hbm.at[pl.ds(y * 4, 4)], parts_ref.at[pl.ds(y * 4, 4)], in_sems.at[y]
        )
        for y in range(4)
    ]
    for load in loads:
        load.start()
    copies = []
    for y in range(4):
        loads[y].wait()
        here = placements(core_ref[0], y, parts_ref, (expand_ref, reduce_ref), sems)
        for copy in here:
            copy.start()
        copies += here
    for copy in copies:
        copy.wait()


def place(core, parts, into):
    _, z, _, r, n = parts.shape
    whole = jax.ShapeDtypeStruct((z, 4, 2, 4, r, n), BF)
    hbm = pl.BlockSpec(memory_space=pl.ANY)
    scratch = [pltpu.SemaphoreType.DMA((32,))]
    if into:
        scratch = [pltpu.VMEM(parts.shape, BF)] + scratch + [pltpu.SemaphoreType.DMA((4,))]
    return pl.pallas_call(
        place_other_kernel if into else place_mine_kernel,
        out_shape=(whole, whole),
        in_specs=[
            pl.BlockSpec(memory_space=pltpu.SMEM),
            hbm if into else pl.BlockSpec(memory_space=pltpu.VMEM),
        ]
        + [hbm] * len(into),
        out_specs=(hbm, hbm),
        scratch_shapes=scratch,
        input_output_aliases={2 + at: at for at in range(len(into))},
        compiler_params=pltpu.CompilerParams(
            vmem_limit_bytes=(60 if into else 8) * 1024 * 1024
        ),
        cost_estimate=pl.CostEstimate(
            flops=parts.size, bytes_accessed=4 * parts.size, transcendentals=0
        ),
    )(core.astype(jnp.int32).reshape(1), parts, *into)


def step(
    acts, saved_hidden, grad_out, master_reduce, master_expand, velocity_reduce, velocity_expand
):
    channels = grad_out.shape[1]
    middle = saved_hidden.shape[1]
    inv_c = 1.0 / float(channels) ** 0.5
    inv_m = 1.0 / float(middle) ** 0.5
    half = jax.ShapeDtypeStruct((16, 8, channels // 256, middle), BF)
    whole = pltpu.VMEM((channels, middle), BF)
    flops = 2 * grad_out.size * middle

    (cur,) = small_call(
        working_kernel,
        (master_expand, master_reduce),
        (jax.ShapeDtypeStruct((8, 2, *master_expand.shape), BF),),
    )
    along_z = exchange(cur, "z")
    mine = everywhere(along_z[:, 0], ("y", "x"))
    keep_e, send_e = local_call(
        functools.partial(expand_kernel, inv_m), (grad_out, saved_hidden), (half, half), [], flops
    )
    (sent_e,) = small_call(chip_sum_kernel, (keep_e, from_other_core(send_e)), (half,))
    other = from_other_core(mine)
    arrived_e = exchange(sent_e, ("y", "x"))
    grad_hidden, keep_r, send_r = local_call(
        functools.partial(hidden_kernel, inv_m, inv_c),
        (saved_hidden, mine, other),
        (jax.ShapeDtypeStruct(saved_hidden.shape, BF), half, half),
        [whole],
        2 * flops,
        (grad_out, acts),
    )
    (sent_r,) = small_call(chip_sum_kernel, (keep_r, from_other_core(send_r)), (half,))
    arrived_r = exchange(sent_r, ("y", "x"))
    row = lax.optimization_barrier(shifted(along_z[:, 1], "x"))
    plane_e = jnp.sum(arrived_e.astype(F32), axis=0).astype(BF)
    (over_plane,) = small_call(
        plane_sum_kernel,
        (plane_e, arrived_r),
        (jax.ShapeDtypeStruct((8, 2, channels // 256, middle), BF),),
    )
    arrived = exchange(over_plane, "z")
    mine_reduce = shifted(row, "y").reshape(half.shape)
    other_reduce = from_other_core(mine_reduce)
    (grad_in,) = local_call(
        functools.partial(back_kernel, inv_c),
        (grad_out, grad_hidden, mine_reduce, other_reduce),
        (jax.ShapeDtypeStruct(grad_out.shape, BF),),
        [whole],
        flops,
    )

    state = (master_expand, master_reduce, velocity_expand, velocity_reduce)
    own = jax.ShapeDtypeStruct(master_expand.shape, F32)
    grads, rows = small_call(
        owner_kernel,
        (arrived, *state),
        (
            jax.ShapeDtypeStruct((2, *own.shape), F32),
            jax.ShapeDtypeStruct((8, 5, *own.shape), BF),
        ),
    )
    ring = exchange(rows, "z")
    (squares,) = small_call(
        ring_squares_kernel, (ring,), (jax.ShapeDtypeStruct((32, 8, 128), F32),)
    )
    squares = exchange(squares, ("y", "c", "x"))
    new_me, new_mr, new_ve, new_vr, work = small_call(
        update_kernel,
        (squares, ring, grads, *state),
        (own, own, own, own, jax.ShapeDtypeStruct((8, 2, *own.shape), BF)),
    )
    mine = everywhere(work, ("y", "x"))
    core = lax.axis_index("c")
    other = from_other_core(mine)
    placed = place(core, mine, ())
    placed = place(1 - core, other, placed)
    work_expand, work_reduce = (p.reshape(channels, middle) for p in placed)
    return (grad_in, new_mr, new_me, new_vr, new_ve, work_reduce, work_expand)


def solution(mesh):
    finer = Mesh(mesh.devices.reshape(8, 4, 2, 4), ROWS_OVER)
    split = P(ROWS_OVER, None)
    return jax.shard_map(
        step,
        mesh=finer,
        in_specs=(split,) * 7,
        out_specs=(split,) * 5 + (P(), P()),
        check_vma=False,
    )
```

```python
import functools

import jax
import jax.numpy as jnp
from jax import lax
from jax.experimental import pallas as pl
from jax.experimental.pallas import tpu as pltpu
from jax.sharding import Mesh
from jax.sharding import PartitionSpec as P


ROWS_OVER = ("z", "y", "c", "x")
BF = jnp.bfloat16
F32 = jnp.float32


def exchange(parts, axes):
    return lax.all_to_all(parts, axes, 0, 0, tiled=True)


def everywhere(block, axes):
    peers = lax.axis_size(axes)
    return exchange(jnp.broadcast_to(block[None], (peers, *block.shape)), axes)


def shifts(block, axis):
    pieces = [block]
    for s in range(1, 4):
        pieces.append(lax.ppermute(block, axis, [(i, (i + s) % 4) for i in range(4)]))
    return pieces


def shifted(block, axis):
    return jnp.concatenate(shifts(block, axis))


def from_other_core(block):
    return lax.ppermute(block, "c", [(0, 1), (1, 0)])


def fill_weights(core, piece, mine_ref, other_ref, whole_ref):
    for z in range(8):
        tiles = []
        for y in range(4):
            at = [piece(y, x) for x in range(4)]
            mine = [mine_ref[i, z].astype(F32) for i in at]
            other = [other_ref[i, z].astype(F32) for i in at]
            tiles += [jnp.where(core == 0, m, o) for m, o in zip(mine, other)]
            tiles += [jnp.where(core == 0, o, m) for m, o in zip(mine, other)]
        rows = jnp.concatenate(tiles, axis=0).astype(BF)
        whole_ref[pl.ds(z * 256, 256), :] = rows


def terms_to_halves(core, left_ref, right, scale, keep_ref, send_ref):
    for z in range(8):
        left = left_ref[:, pl.ds(z * 256, 256)]
        part = lax.dot_general(left, right, (((0,), (0,)), ((), ())), preferred_element_type=F32)
        part = (part * scale).reshape(4, 2, 4, 8, right.shape[1])
        for y in range(4):
            first, second = part[y, 0], part[y, 1]
            keep_ref[pl.ds(y * 4, 4), z] = jnp.where(core == 0, first, second).astype(BF)
            send_ref[pl.ds(y * 4, 4), z] = jnp.where(core == 0, second, first).astype(BF)


def expand_kernel(scale, place_ref, grad_ref, hidden_ref, keep_ref, send_ref):
    terms_to_halves(place_ref[0], grad_ref, hidden_ref[...], scale, keep_ref, send_ref)


def hidden_kernel(
    inv_m,
    inv_c,
    place_ref,
    saved_ref,
    mine_ref,
    other_ref,
    grad_hbm,
    acts_hbm,
    out_ref,
    keep_ref,
    send_ref,
    whole_ref,
    grad_ref,
    acts_ref,
    sems,
):
    core = place_ref[0]
    grad_copy = pltpu.make_async_copy(grad_hbm, grad_ref, sems.at[0])
    acts_copy = pltpu.make_async_copy(acts_hbm, acts_ref, sems.at[1])
    grad_copy.start()
    acts_copy.start()
    fill_weights(core, lambda y, x: y * 4 + x, mine_ref, other_ref, whole_ref)
    grad_copy.wait()
    summed = jnp.dot(grad_ref[...], whole_ref[...], preferred_element_type=F32)
    saved = saved_ref[...].astype(F32)
    out_ref[...] = jnp.where(saved > 0, summed * inv_m, 0.0).astype(BF)
    acts_copy.wait()
    terms_to_halves(core, acts_ref, out_ref[...], inv_c, keep_ref, send_ref)


def working_kernel(me_ref, mr_ref, out_ref):
    for layer, m_ref in enumerate((me_ref, mr_ref)):
        rows = m_ref[...].astype(BF)
        for z in range(8):
            out_ref[z, layer] = rows


def chip_sum_kernel(keep_ref, got_ref, out_ref):
    out_ref[...] = (keep_ref[...].astype(F32) + got_ref[...].astype(F32)).astype(BF)


def plane_sum_kernel(expand_ref, reduce_ref, out_ref):
    for z in range(8):
        out_ref[z, 0] = expand_ref[z]
        total = reduce_ref[0, z].astype(F32)
        for peer in range(1, reduce_ref.shape[0]):
            total = total + reduce_ref[peer, z].astype(F32)
        out_ref[z, 1] = total.astype(BF)


def back_kernel(inv_c, place_ref, grad_ref, hidden_ref, mine_ref, other_ref, out_ref, whole_ref):
    core, my_y, my_x = place_ref[0], place_ref[1], place_ref[2]

    def piece(y, x):
        return lax.rem(my_y - y + 4, 4) * 4 + lax.rem(my_x - x + 4, 4)

    fill_weights(core, piece, mine_ref, other_ref, whole_ref)
    for z in range(8):
        columns = pl.ds(z * 256, 256)
        back = lax.dot_general(
            hidden_ref[...],
            whole_ref[columns, :],
            (((1,), (1,)), ((), ())),
            preferred_element_type=F32,
        )
        out_ref[:, columns] = (grad_ref[:, columns].astype(F32) + back * inv_c).astype(BF)


def local_call(kernel, operands, outs, scratch, flops, streamed=()):
    whole = pl.BlockSpec(memory_space=pltpu.VMEM)
    at = jnp.stack([lax.axis_index(axis).astype(jnp.int32) for axis in ("c", "y", "x")])
    moved = sum(x.size * x.dtype.itemsize for x in (*operands, *streamed, *outs))
    scratch = scratch + [pltpu.VMEM(x.shape, x.dtype) for x in streamed]
    if streamed:
        scratch = scratch + [pltpu.SemaphoreType.DMA((len(streamed),))]
    return pl.pallas_call(
        kernel,
        out_shape=outs,
        in_specs=[pl.BlockSpec(memory_space=pltpu.SMEM)] + [whole] * len(operands)
        + [pl.BlockSpec(memory_space=pltpu.HBM)] * len(streamed),
        out_specs=[whole] * len(outs),
        scratch_shapes=scratch,
        compiler_params=pltpu.CompilerParams(vmem_limit_bytes=50 * 1024 * 1024),
        cost_estimate=pl.CostEstimate(flops=flops, bytes_accessed=moved, transcendentals=0),
    )(at, *operands, *streamed)


def total_of(terms):
    return jnp.sum(jnp.sum(terms, axis=1, keepdims=True), axis=0, keepdims=True)


def owner_kernel(arrived_ref, me_ref, mr_ref, ve_ref, vr_ref, grads_ref, out_ref):
    tiles, squares = [], []
    moved = []
    for layer, (m_ref, v_ref) in enumerate(((me_ref, ve_ref), (mr_ref, vr_ref))):
        grads = arrived_ref[0, layer].astype(F32)
        for z in range(1, 8):
            grads = grads + arrived_ref[z, layer].astype(F32)
        grads_ref[layer] = grads
        master = m_ref[...]
        tiles.append((grads + 5e-05 * master).astype(BF))
        moved.append((master - 0.1 * (0.9 * v_ref[...])).astype(BF))
        squares += [total_of(master * master), total_of(grads * grads)]
    tiles += moved
    rows = lax.broadcasted_iota(jnp.int32, (8, 128), 0)
    left = jnp.zeros((8, 128), F32)
    for at, square in enumerate(squares):
        left = jnp.where(rows == at, square, left)
    parts = []
    for _ in range(3):
        part = left.astype(BF)
        left = left - part.astype(F32)
        parts.append(part)
    tiles.append(jnp.concatenate(parts + [jnp.zeros((8, 128), BF)], axis=1))
    for z in range(8):
        for at, tile in enumerate(tiles):
            out_ref[z, at] = tile


def ring_squares_kernel(ring_ref, out_ref, low_ref, high_ref):
    total = jnp.zeros((8, 128), F32)
    for z in range(8):
        packed = ring_ref[z, 4].astype(F32)
        total = total + ((packed[:, :128] + packed[:, 128:256]) + packed[:, 256:384])
        half_ref = low_ref if z < 4 else high_ref
        half_ref[z % 4] = ring_ref[z, :4]
    out_ref[...] = jnp.broadcast_to(total[None], out_ref.shape)


def update_kernel(
    squares_ref,
    grads_ref,
    me_ref,
    mr_ref,
    ve_ref,
    vr_ref,
    *refs,
):
    low_refs, high_refs = refs[:4], refs[4:8]
    new_me_ref, new_mr_ref, new_ve_ref, new_vr_ref, low_work_ref, high_work_ref = refs[8:]
    squares = squares_ref[0]
    for peer in range(1, squares_ref.shape[0]):
        squares = squares + squares_ref[peer]
    norms = jnp.sqrt(squares)
    layers = (
        (me_ref, ve_ref, new_me_ref, new_ve_ref),
        (mr_ref, vr_ref, new_mr_ref, new_vr_ref),
    )
    for layer, (m_ref, v_ref, new_m_ref, new_v_ref) in enumerate(layers):
        wnorm = norms[2 * layer : 2 * layer + 1, :1]
        gnorm = norms[2 * layer + 1 : 2 * layer + 2, :1]
        trust = wnorm / (gnorm + 5e-05 * wnorm)
        master = m_ref[...]
        new_velocity = 0.9 * v_ref[...] + trust * (grads_ref[layer] + 5e-05 * master)
        new_v_ref[...] = new_velocity
        new_m_ref[...] = master - 0.1 * new_velocity
        for half_refs, work_ref in ((low_refs, low_work_ref), (high_refs, high_work_ref)):
            for s, half_ref in enumerate(half_refs):
                for z in range(4):
                    step = 0.1 * (trust * half_ref[z, layer].astype(F32))
                    work_ref[s, z, layer] = (half_ref[z, 2 + layer].astype(F32) - step).astype(BF)


def small_call(kernel, operands, outs, limit=16):
    whole = pl.BlockSpec(memory_space=pltpu.VMEM)
    moved = sum(x.size * x.dtype.itemsize for x in (*operands, *outs))
    return pl.pallas_call(
        kernel,
        out_shape=outs,
        in_specs=[whole] * len(operands),
        out_specs=[whole] * len(outs),
        compiler_params=pltpu.CompilerParams(vmem_limit_bytes=limit * 1024 * 1024),
        cost_estimate=pl.CostEstimate(flops=moved, bytes_accessed=moved, transcendentals=0),
    )(*operands)


def placements(at_ref, core, half, i, parts_ref, out_refs, sems):
    copies = []
    for j in range(4):
        x = lax.rem(at_ref[2] - (i if half else j) + 4, 4)
        y = lax.rem(at_ref[1] - j + 4, 4) if half else i
        for layer, out_ref in enumerate(out_refs):
            copies.append(
                pltpu.make_async_copy(
                    parts_ref.at[i, j, :, layer],
                    out_ref.at[pl.ds(half * 4, 4), y, core, x],
                    sems.at[half * 32 + i * 8 + j * 2 + layer],
                )
            )
    return copies


def place_kernel(other, at_ref, low_ref, high_ref, *refs):
    expand_ref, reduce_ref, sems = refs[-3:]
    core = 1 - at_ref[0] if other else at_ref[0]
    copies = []
    for half, parts_ref in enumerate((low_ref, high_ref)):
        for i in range(4):
            copies += placements(at_ref, core, half, i, parts_ref, (expand_ref, reduce_ref), sems)
    for copy in copies:
        copy.start()
    for copy in copies:
        copy.wait()


def place(halves, into):
    _, _, z, _, r, n = halves[0].shape
    whole = jax.ShapeDtypeStruct((2 * z, 4, 2, 4, r, n), BF)
    hbm = pl.BlockSpec(memory_space=pl.ANY)
    at = jnp.stack([lax.axis_index(axis).astype(jnp.int32) for axis in ("c", "y", "x")])
    return pl.pallas_call(
        functools.partial(place_kernel, bool(into)),
        out_shape=(whole, whole),
        in_specs=[pl.BlockSpec(memory_space=pltpu.SMEM)]
        + [pl.BlockSpec(memory_space=pltpu.VMEM)] * 2
        + [hbm] * len(into),
        out_specs=(hbm, hbm),
        scratch_shapes=[pltpu.SemaphoreType.DMA((64,))],
        input_output_aliases={3 + at: at for at in range(len(into))},
        compiler_params=pltpu.CompilerParams(
            vmem_limit_bytes=8 * 1024 * 1024
        ),
        cost_estimate=pl.CostEstimate(
            flops=halves[0].size, bytes_accessed=8 * halves[0].size, transcendentals=0
        ),
    )(at, *halves, *into)


def step(
    acts, saved_hidden, grad_out, master_reduce, master_expand, velocity_reduce, velocity_expand
):
    channels = grad_out.shape[1]
    middle = saved_hidden.shape[1]
    inv_c = 1.0 / float(channels) ** 0.5
    inv_m = 1.0 / float(middle) ** 0.5
    half = jax.ShapeDtypeStruct((16, 8, channels // 256, middle), BF)
    whole = pltpu.VMEM((channels, middle), BF)
    flops = 2 * grad_out.size * middle

    (cur,) = small_call(
        working_kernel,
        (master_expand, master_reduce),
        (jax.ShapeDtypeStruct((8, 2, *master_expand.shape), BF),),
        60,
    )
    along_z = exchange(cur, "z")
    mine = everywhere(along_z[:, 0], ("y", "x"))
    keep_e, send_e = local_call(
        functools.partial(expand_kernel, inv_m), (grad_out, saved_hidden), (half, half), [], flops
    )
    (sent_e,) = small_call(chip_sum_kernel, (keep_e, from_other_core(send_e)), (half,))
    other = from_other_core(mine)
    arrived_e = exchange(sent_e, ("y", "x"))
    grad_hidden, keep_r, send_r = local_call(
        functools.partial(hidden_kernel, inv_m, inv_c),
        (saved_hidden, mine, other),
        (jax.ShapeDtypeStruct(saved_hidden.shape, BF), half, half),
        [whole],
        2 * flops,
        (grad_out, acts),
    )
    (sent_r,) = small_call(chip_sum_kernel, (keep_r, from_other_core(send_r)), (half,))
    arrived_r = exchange(sent_r, ("y", "x"))
    row = lax.optimization_barrier(shifted(along_z[:, 1], "x"))
    plane_e = jnp.sum(arrived_e.astype(F32), axis=0).astype(BF)
    (over_plane,) = small_call(
        plane_sum_kernel,
        (plane_e, arrived_r),
        (jax.ShapeDtypeStruct((8, 2, channels // 256, middle), BF),),
    )
    arrived = exchange(over_plane, "z")
    mine_reduce = shifted(row, "y").reshape(half.shape)
    other_reduce = from_other_core(mine_reduce)
    (grad_in,) = local_call(
        functools.partial(back_kernel, inv_c),
        (grad_out, grad_hidden, mine_reduce, other_reduce),
        (jax.ShapeDtypeStruct(grad_out.shape, BF),),
        [whole],
        flops,
    )

    state = (master_expand, master_reduce, velocity_expand, velocity_reduce)
    own = jax.ShapeDtypeStruct(master_expand.shape, F32)
    grads, rows = small_call(
        owner_kernel,
        (arrived, *state),
        (
            jax.ShapeDtypeStruct((2, *own.shape), F32),
            jax.ShapeDtypeStruct((8, 5, *own.shape), BF),
        ),
    )
    ring = exchange(rows, "z")
    quarter = jax.ShapeDtypeStruct((4, 4, *own.shape), BF)
    squares, low, high = small_call(
        ring_squares_kernel,
        (ring,),
        (jax.ShapeDtypeStruct((32, 8, 128), F32), quarter, quarter),
    )
    squares = exchange(squares, ("y", "c", "x"))
    lows = shifts(low, "x")
    highs = shifts(high, "y")
    four = jax.ShapeDtypeStruct((4, 4, 2, *own.shape), BF)
    new_me, new_mr, new_ve, new_vr, low_work, high_work = small_call(
        update_kernel,
        (squares, grads, *state, *lows, *highs),
        (own, own, own, own, four, four),
    )
    low_mine = everywhere(low_work, "y")
    high_mine = jnp.stack(shifts(high_work, "x"))
    low_other = from_other_core(low_mine)
    high_other = from_other_core(high_mine)
    placed = place((low_mine, high_mine), ())
    placed = place((low_other, high_other), placed)
    work_expand, work_reduce = (p.reshape(channels, middle) for p in placed)
    return (grad_in, new_mr, new_me, new_vr, new_ve, work_reduce, work_expand)


def solution(mesh):
    finer = Mesh(mesh.devices.reshape(8, 4, 2, 4), ROWS_OVER)
    split = P(ROWS_OVER, None)
    return jax.shard_map(
        step,
        mesh=finer,
        in_specs=(split,) * 7,
        out_specs=(split,) * 5 + (P(), P()),
        check_vma=False,
    )
```

```python
import functools

import jax
import jax.numpy as jnp
from jax import lax
from jax.experimental import pallas as pl
from jax.experimental.pallas import tpu as pltpu
from jax.sharding import Mesh
from jax.sharding import PartitionSpec as P


ROWS_OVER = ("z", "y", "c", "x")
BF = jnp.bfloat16
F32 = jnp.float32


def exchange(parts, axes):
    return lax.all_to_all(parts, axes, 0, 0, tiled=True)


def everywhere(block, axes):
    peers = lax.axis_size(axes)
    return exchange(jnp.broadcast_to(block[None], (peers, *block.shape)), axes)


def shifts(block, axis):
    pieces = [block]
    for s in range(1, 4):
        pieces.append(lax.ppermute(block, axis, [(i, (i + s) % 4) for i in range(4)]))
    return pieces


def shifted(block, axis):
    return jnp.concatenate(shifts(block, axis))


def from_other_core(block):
    return lax.ppermute(block, "c", [(0, 1), (1, 0)])


def fill_weights(core, piece, mine_ref, other_ref, whole_ref):
    for z in range(8):
        tiles = []
        for y in range(4):
            at = [piece(y, x) for x in range(4)]
            mine = [mine_ref[i, z].astype(F32) for i in at]
            other = [other_ref[i, z].astype(F32) for i in at]
            tiles += [jnp.where(core == 0, m, o) for m, o in zip(mine, other)]
            tiles += [jnp.where(core == 0, o, m) for m, o in zip(mine, other)]
        rows = jnp.concatenate(tiles, axis=0).astype(BF)
        whole_ref[pl.ds(z * 256, 256), :] = rows


def terms_to_halves(core, left_ref, right, scale, keep_ref, send_ref):
    for z in range(8):
        left = left_ref[:, pl.ds(z * 256, 256)]
        part = lax.dot_general(left, right, (((0,), (0,)), ((), ())), preferred_element_type=F32)
        part = (part * scale).reshape(4, 2, 4, 8, right.shape[1])
        for y in range(4):
            first, second = part[y, 0], part[y, 1]
            keep_ref[pl.ds(y * 4, 4), z] = jnp.where(core == 0, first, second).astype(BF)
            send_ref[pl.ds(y * 4, 4), z] = jnp.where(core == 0, second, first).astype(BF)


def expand_kernel(scale, place_ref, grad_ref, hidden_ref, keep_ref, send_ref):
    terms_to_halves(place_ref[0], grad_ref, hidden_ref[...], scale, keep_ref, send_ref)


def hidden_kernel(
    inv_m,
    inv_c,
    place_ref,
    saved_ref,
    mine_ref,
    other_ref,
    grad_hbm,
    acts_hbm,
    out_ref,
    keep_ref,
    send_ref,
    whole_ref,
    grad_ref,
    acts_ref,
    sems,
):
    core = place_ref[0]
    grad_copy = pltpu.make_async_copy(grad_hbm, grad_ref, sems.at[0])
    acts_copy = pltpu.make_async_copy(acts_hbm, acts_ref, sems.at[1])
    grad_copy.start()
    acts_copy.start()
    fill_weights(core, lambda y, x: y * 4 + x, mine_ref, other_ref, whole_ref)
    grad_copy.wait()
    summed = jnp.dot(grad_ref[...], whole_ref[...], preferred_element_type=F32)
    saved = saved_ref[...].astype(F32)
    out_ref[...] = jnp.where(saved > 0, summed * inv_m, 0.0).astype(BF)
    acts_copy.wait()
    terms_to_halves(core, acts_ref, out_ref[...], inv_c, keep_ref, send_ref)


def working_kernel(me_ref, mr_ref, out_ref):
    for layer, m_ref in enumerate((me_ref, mr_ref)):
        rows = m_ref[...].astype(BF)
        for z in range(8):
            out_ref[z, layer] = rows


def chip_sum_kernel(keep_ref, got_ref, out_ref):
    out_ref[...] = (keep_ref[...].astype(F32) + got_ref[...].astype(F32)).astype(BF)


def plane_sum_kernel(expand_ref, reduce_ref, out_ref):
    for z in range(8):
        out_ref[z, 0] = expand_ref[z]
        total = reduce_ref[0, z].astype(F32)
        for peer in range(1, reduce_ref.shape[0]):
            total = total + reduce_ref[peer, z].astype(F32)
        out_ref[z, 1] = total.astype(BF)


def back_kernel(inv_c, place_ref, grad_ref, hidden_ref, mine_ref, other_ref, out_ref, whole_ref):
    core, my_y, my_x = place_ref[0], place_ref[1], place_ref[2]

    def piece(y, x):
        return lax.rem(my_y - y + 4, 4) * 4 + lax.rem(my_x - x + 4, 4)

    fill_weights(core, piece, mine_ref, other_ref, whole_ref)
    for z in range(8):
        columns = pl.ds(z * 256, 256)
        back = lax.dot_general(
            hidden_ref[...],
            whole_ref[columns, :],
            (((1,), (1,)), ((), ())),
            preferred_element_type=F32,
        )
        out_ref[:, columns] = (grad_ref[:, columns].astype(F32) + back * inv_c).astype(BF)


def local_call(kernel, operands, outs, scratch, flops, streamed=(), limit=50):
    whole = pl.BlockSpec(memory_space=pltpu.VMEM)
    at = jnp.stack([lax.axis_index(axis).astype(jnp.int32) for axis in ("c", "y", "x")])
    moved = sum(x.size * x.dtype.itemsize for x in (*operands, *streamed, *outs))
    scratch = scratch + [pltpu.VMEM(x.shape, x.dtype) for x in streamed]
    if streamed:
        scratch = scratch + [pltpu.SemaphoreType.DMA((len(streamed),))]
    return pl.pallas_call(
        kernel,
        out_shape=outs,
        in_specs=[pl.BlockSpec(memory_space=pltpu.SMEM)] + [whole] * len(operands)
        + [pl.BlockSpec(memory_space=pltpu.HBM)] * len(streamed),
        out_specs=[whole] * len(outs),
        scratch_shapes=scratch,
        compiler_params=pltpu.CompilerParams(vmem_limit_bytes=limit * 1024 * 1024),
        cost_estimate=pl.CostEstimate(flops=flops, bytes_accessed=moved, transcendentals=0),
    )(at, *operands, *streamed)


def total_of(terms):
    return jnp.sum(jnp.sum(terms, axis=1, keepdims=True), axis=0, keepdims=True)


def owner_kernel(arrived_ref, me_ref, mr_ref, ve_ref, vr_ref, grads_ref, out_ref):
    tiles, squares = [], []
    moved = []
    for layer, (m_ref, v_ref) in enumerate(((me_ref, ve_ref), (mr_ref, vr_ref))):
        grads = arrived_ref[0, layer].astype(F32)
        for z in range(1, 8):
            grads = grads + arrived_ref[z, layer].astype(F32)
        grads_ref[layer] = grads
        master = m_ref[...]
        tiles.append((grads + 5e-05 * master).astype(BF))
        moved.append((master - 0.1 * (0.9 * v_ref[...])).astype(BF))
        squares += [total_of(master * master), total_of(grads * grads)]
    tiles += moved
    rows = lax.broadcasted_iota(jnp.int32, (8, 128), 0)
    left = jnp.zeros((8, 128), F32)
    for at, square in enumerate(squares):
        left = jnp.where(rows == at, square, left)
    parts = []
    for _ in range(3):
        part = left.astype(BF)
        left = left - part.astype(F32)
        parts.append(part)
    tiles.append(jnp.concatenate(parts + [jnp.zeros((8, 128), BF)], axis=1))
    for z in range(8):
        for at, tile in enumerate(tiles):
            out_ref[z, at] = tile


def ring_squares_kernel(ring_ref, out_ref, low_ref, high_ref):
    total = jnp.zeros((8, 128), F32)
    for z in range(8):
        packed = ring_ref[z, 4].astype(F32)
        total = total + ((packed[:, :128] + packed[:, 128:256]) + packed[:, 256:384])
        half_ref = low_ref if z < 4 else high_ref
        half_ref[z % 4] = ring_ref[z, :4]
    out_ref[...] = jnp.broadcast_to(total[None], out_ref.shape)


def update_kernel(
    squares_ref,
    grads_ref,
    me_ref,
    mr_ref,
    ve_ref,
    vr_ref,
    *refs,
):
    low_refs, high_refs = refs[:4], refs[4:8]
    new_me_ref, new_mr_ref, new_ve_ref, new_vr_ref, low_work_ref, high_work_ref = refs[8:]
    squares = squares_ref[0]
    for peer in range(1, squares_ref.shape[0]):
        squares = squares + squares_ref[peer]
    norms = jnp.sqrt(squares)
    layers = (
        (me_ref, ve_ref, new_me_ref, new_ve_ref),
        (mr_ref, vr_ref, new_mr_ref, new_vr_ref),
    )
    for layer, (m_ref, v_ref, new_m_ref, new_v_ref) in enumerate(layers):
        wnorm = norms[2 * layer : 2 * layer + 1, :1]
        gnorm = norms[2 * layer + 1 : 2 * layer + 2, :1]
        trust = wnorm / (gnorm + 5e-05 * wnorm)
        master = m_ref[...]
        new_velocity = 0.9 * v_ref[...] + trust * (grads_ref[layer] + 5e-05 * master)
        new_v_ref[...] = new_velocity
        new_m_ref[...] = master - 0.1 * new_velocity
        for half_refs, work_ref in ((low_refs, low_work_ref), (high_refs, high_work_ref)):
            for s, half_ref in enumerate(half_refs):
                for z in range(4):
                    step = 0.1 * (trust * half_ref[z, layer].astype(F32))
                    work_ref[s, z, layer] = (half_ref[z, 2 + layer].astype(F32) - step).astype(BF)


def small_call(kernel, operands, outs, limit=16):
    whole = pl.BlockSpec(memory_space=pltpu.VMEM)
    moved = sum(x.size * x.dtype.itemsize for x in (*operands, *outs))
    return pl.pallas_call(
        kernel,
        out_shape=outs,
        in_specs=[whole] * len(operands),
        out_specs=[whole] * len(outs),
        compiler_params=pltpu.CompilerParams(vmem_limit_bytes=limit * 1024 * 1024),
        cost_estimate=pl.CostEstimate(flops=moved, bytes_accessed=moved, transcendentals=0),
    )(*operands)


def placements(at_ref, core, half, i, parts_ref, out_refs, sems):
    copies = []
    for j in range(4):
        x = lax.rem(at_ref[2] - (i if half else j) + 4, 4)
        y = lax.rem(at_ref[1] - j + 4, 4) if half else i
        for layer, out_ref in enumerate(out_refs):
            copies.append(
                pltpu.make_async_copy(
                    parts_ref.at[i, j, :, layer],
                    out_ref.at[pl.ds(half * 4, 4), y, core, x],
                    sems.at[half * 32 + i * 8 + j * 2 + layer],
                )
            )
    return copies


def place_kernel(other, halves, at_ref, *refs):
    expand_ref, reduce_ref, sems = refs[-3:]
    core = 1 - at_ref[0] if other else at_ref[0]
    copies = []
    for half, parts_ref in zip(halves, refs):
        for i in range(4):
            copies += placements(at_ref, core, half, i, parts_ref, (expand_ref, reduce_ref), sems)
    for copy in copies:
        copy.start()
    for copy in copies:
        copy.wait()


def place(other, halves, parts, into):
    _, _, z, _, r, n = parts[0].shape
    whole = jax.ShapeDtypeStruct((2 * z, 4, 2, 4, r, n), BF)
    hbm = pl.BlockSpec(memory_space=pl.ANY)
    at = jnp.stack([lax.axis_index(axis).astype(jnp.int32) for axis in ("c", "y", "x")])
    first = 1 + len(parts)
    return pl.pallas_call(
        functools.partial(place_kernel, other, halves),
        out_shape=(whole, whole),
        in_specs=[pl.BlockSpec(memory_space=pltpu.SMEM)]
        + [pl.BlockSpec(memory_space=pltpu.VMEM)] * len(parts)
        + [hbm] * len(into),
        out_specs=(hbm, hbm),
        scratch_shapes=[pltpu.SemaphoreType.DMA((64,))],
        input_output_aliases={first + at: at for at in range(len(into))},
        compiler_params=pltpu.CompilerParams(vmem_limit_bytes=8 * 1024 * 1024),
        cost_estimate=pl.CostEstimate(
            flops=parts[0].size, bytes_accessed=4 * len(parts) * parts[0].size, transcendentals=0
        ),
    )(at, *parts, *into)


def step(
    acts, saved_hidden, grad_out, master_reduce, master_expand, velocity_reduce, velocity_expand
):
    channels = grad_out.shape[1]
    middle = saved_hidden.shape[1]
    inv_c = 1.0 / float(channels) ** 0.5
    inv_m = 1.0 / float(middle) ** 0.5
    half = jax.ShapeDtypeStruct((16, 8, channels // 256, middle), BF)
    whole = pltpu.VMEM((channels, middle), BF)
    flops = 2 * grad_out.size * middle

    (cur,) = small_call(
        working_kernel,
        (master_expand, master_reduce),
        (jax.ShapeDtypeStruct((8, 2, *master_expand.shape), BF),),
        60,
    )
    along_z = exchange(cur, "z")
    mine = everywhere(along_z[:, 0], ("y", "x"))
    keep_e, send_e = local_call(
        functools.partial(expand_kernel, inv_m), (grad_out, saved_hidden), (half, half), [], flops
    )
    (sent_e,) = small_call(chip_sum_kernel, (keep_e, from_other_core(send_e)), (half,))
    other = from_other_core(mine)
    arrived_e = exchange(sent_e, ("y", "x"))
    grad_hidden, keep_r, send_r = local_call(
        functools.partial(hidden_kernel, inv_m, inv_c),
        (saved_hidden, mine, other),
        (jax.ShapeDtypeStruct(saved_hidden.shape, BF), half, half),
        [whole],
        2 * flops,
        (grad_out, acts),
    )
    (sent_r,) = small_call(chip_sum_kernel, (keep_r, from_other_core(send_r)), (half,))
    arrived_r = exchange(sent_r, ("y", "x"))
    row = lax.optimization_barrier(shifted(along_z[:, 1], "x"))
    plane_e = jnp.sum(arrived_e.astype(F32), axis=0).astype(BF)
    (over_plane,) = small_call(
        plane_sum_kernel,
        (plane_e, arrived_r),
        (jax.ShapeDtypeStruct((8, 2, channels // 256, middle), BF),),
    )
    arrived = exchange(over_plane, "z")
    mine_reduce = shifted(row, "y").reshape(half.shape)
    other_reduce = from_other_core(mine_reduce)
    (grad_in,) = local_call(
        functools.partial(back_kernel, inv_c),
        (grad_out, grad_hidden, mine_reduce, other_reduce),
        (jax.ShapeDtypeStruct(grad_out.shape, BF),),
        [whole],
        flops,
        limit=62,
    )

    state = (master_expand, master_reduce, velocity_expand, velocity_reduce)
    own = jax.ShapeDtypeStruct(master_expand.shape, F32)
    grads, rows = small_call(
        owner_kernel,
        (arrived, *state),
        (
            jax.ShapeDtypeStruct((2, *own.shape), F32),
            jax.ShapeDtypeStruct((8, 5, *own.shape), BF),
        ),
    )
    ring = exchange(rows, "z")
    quarter = jax.ShapeDtypeStruct((4, 4, *own.shape), BF)
    squares, low, high = small_call(
        ring_squares_kernel,
        (ring,),
        (jax.ShapeDtypeStruct((32, 8, 128), F32), quarter, quarter),
    )
    squares = exchange(squares, ("y", "c", "x"))
    lows = shifts(low, "x")
    highs = shifts(high, "y")
    four = jax.ShapeDtypeStruct((4, 4, 2, *own.shape), BF)
    new_me, new_mr, new_ve, new_vr, low_work, high_work = small_call(
        update_kernel,
        (squares, grads, *state, *lows, *highs),
        (own, own, own, own, four, four),
    )
    low_mine = everywhere(low_work, "y")
    high_mine = jnp.stack(shifts(high_work, "x"))
    low_other = from_other_core(low_mine)
    high_other = from_other_core(high_mine)
    placed = place(False, (0, 1), (low_mine, high_mine), ())
    placed = place(True, (1,), (high_other,), placed)
    placed = place(True, (0,), (low_other,), placed)
    work_expand, work_reduce = (p.reshape(channels, middle) for p in placed)
    return (grad_in, new_mr, new_me, new_vr, new_ve, work_reduce, work_expand)


def solution(mesh):
    finer = Mesh(mesh.devices.reshape(8, 4, 2, 4), ROWS_OVER)
    split = P(ROWS_OVER, None)
    return jax.shard_map(
        step,
        mesh=finer,
        in_specs=(split,) * 7,
        out_specs=(split,) * 5 + (P(), P()),
        check_vma=False,
    )
```

```python
import functools

import jax
import jax.numpy as jnp
from jax import lax
from jax.experimental import pallas as pl
from jax.experimental.pallas import tpu as pltpu
from jax.sharding import Mesh
from jax.sharding import PartitionSpec as P


ROWS_OVER = ("z", "y", "c", "x")
BF = jnp.bfloat16
F32 = jnp.float32


def exchange(parts, axes):
    return lax.all_to_all(parts, axes, 0, 0, tiled=True)


def everywhere(block, axes):
    peers = lax.axis_size(axes)
    return exchange(jnp.broadcast_to(block[None], (peers, *block.shape)), axes)


def shifts(block, axis):
    pieces = [block]
    for s in range(1, 4):
        pieces.append(lax.ppermute(block, axis, [(i, (i + s) % 4) for i in range(4)]))
    return pieces


def shifted(block, axis):
    return jnp.concatenate(shifts(block, axis))


def from_other_core(block):
    return lax.ppermute(block, "c", [(0, 1), (1, 0)])


def fill_weights(core, piece, mine_ref, other_ref, whole_ref):
    for z in range(8):
        tiles = []
        for y in range(4):
            at = [piece(y, x) for x in range(4)]
            mine = [mine_ref[i, z].astype(F32) for i in at]
            other = [other_ref[i, z].astype(F32) for i in at]
            tiles += [jnp.where(core == 0, m, o) for m, o in zip(mine, other)]
            tiles += [jnp.where(core == 0, o, m) for m, o in zip(mine, other)]
        rows = jnp.concatenate(tiles, axis=0).astype(BF)
        whole_ref[pl.ds(z * 256, 256), :] = rows


def terms_to_halves(core, left_ref, right, scale, keep_ref, send_ref):
    for z in range(8):
        left = left_ref[:, pl.ds(z * 256, 256)]
        part = lax.dot_general(left, right, (((0,), (0,)), ((), ())), preferred_element_type=F32)
        part = (part * scale).reshape(4, 2, 4, 8, right.shape[1])
        for y in range(4):
            first, second = part[y, 0], part[y, 1]
            keep_ref[pl.ds(y * 4, 4), z] = jnp.where(core == 0, first, second).astype(BF)
            send_ref[pl.ds(y * 4, 4), z] = jnp.where(core == 0, second, first).astype(BF)


def expand_kernel(scale, place_ref, grad_ref, hidden_ref, keep_ref, send_ref):
    terms_to_halves(place_ref[0], grad_ref, hidden_ref[...], scale, keep_ref, send_ref)


def hidden_kernel(
    inv_m,
    inv_c,
    place_ref,
    saved_ref,
    mine_ref,
    other_ref,
    grad_hbm,
    acts_hbm,
    out_ref,
    keep_ref,
    send_ref,
    whole_ref,
    grad_ref,
    acts_ref,
    sems,
):
    core = place_ref[0]
    grad_copy = pltpu.make_async_copy(grad_hbm, grad_ref, sems.at[0])
    acts_copy = pltpu.make_async_copy(acts_hbm, acts_ref, sems.at[1])
    grad_copy.start()
    acts_copy.start()
    fill_weights(core, lambda y, x: y * 4 + x, mine_ref, other_ref, whole_ref)
    grad_copy.wait()
    summed = jnp.dot(grad_ref[...], whole_ref[...], preferred_element_type=F32)
    saved = saved_ref[...].astype(F32)
    out_ref[...] = jnp.where(saved > 0, summed * inv_m, 0.0).astype(BF)
    acts_copy.wait()
    terms_to_halves(core, acts_ref, out_ref[...], inv_c, keep_ref, send_ref)


def working_kernel(me_ref, mr_ref, out_ref):
    for layer, m_ref in enumerate((me_ref, mr_ref)):
        rows = m_ref[...].astype(BF)
        for z in range(8):
            out_ref[z, layer] = rows


def chip_sum_kernel(keep_ref, got_ref, out_ref):
    out_ref[...] = (keep_ref[...].astype(F32) + got_ref[...].astype(F32)).astype(BF)


def plane_sum_kernel(expand_ref, reduce_ref, out_ref):
    for z in range(8):
        out_ref[z, 0] = expand_ref[z]
        total = reduce_ref[0, z].astype(F32)
        for peer in range(1, reduce_ref.shape[0]):
            total = total + reduce_ref[peer, z].astype(F32)
        out_ref[z, 1] = total.astype(BF)


def back_kernel(inv_c, place_ref, grad_ref, hidden_ref, mine_ref, other_ref, out_ref, whole_ref):
    core, my_y, my_x = place_ref[0], place_ref[1], place_ref[2]

    def piece(y, x):
        return lax.rem(my_y - y + 4, 4) * 4 + lax.rem(my_x - x + 4, 4)

    fill_weights(core, piece, mine_ref, other_ref, whole_ref)
    for z in range(8):
        columns = pl.ds(z * 256, 256)
        back = lax.dot_general(
            hidden_ref[...],
            whole_ref[columns, :],
            (((1,), (1,)), ((), ())),
            preferred_element_type=F32,
        )
        out_ref[:, columns] = (grad_ref[:, columns].astype(F32) + back * inv_c).astype(BF)


def local_call(kernel, operands, outs, scratch, flops, streamed=(), limit=50):
    whole = pl.BlockSpec(memory_space=pltpu.VMEM)
    at = jnp.stack([lax.axis_index(axis).astype(jnp.int32) for axis in ("c", "y", "x")])
    moved = sum(x.size * x.dtype.itemsize for x in (*operands, *streamed, *outs))
    scratch = scratch + [pltpu.VMEM(x.shape, x.dtype) for x in streamed]
    if streamed:
        scratch = scratch + [pltpu.SemaphoreType.DMA((len(streamed),))]
    return pl.pallas_call(
        kernel,
        out_shape=outs,
        in_specs=[pl.BlockSpec(memory_space=pltpu.SMEM)] + [whole] * len(operands)
        + [pl.BlockSpec(memory_space=pltpu.HBM)] * len(streamed),
        out_specs=[whole] * len(outs),
        scratch_shapes=scratch,
        compiler_params=pltpu.CompilerParams(vmem_limit_bytes=limit * 1024 * 1024),
        cost_estimate=pl.CostEstimate(flops=flops, bytes_accessed=moved, transcendentals=0),
    )(at, *operands, *streamed)


def total_of(terms):
    return jnp.sum(jnp.sum(terms, axis=1, keepdims=True), axis=0, keepdims=True)


def owner_kernel(arrived_ref, me_ref, mr_ref, ve_ref, vr_ref, grads_ref, out_ref):
    tiles, squares = [], []
    moved = []
    for layer, (m_ref, v_ref) in enumerate(((me_ref, ve_ref), (mr_ref, vr_ref))):
        grads = arrived_ref[0, layer].astype(F32)
        for z in range(1, 8):
            grads = grads + arrived_ref[z, layer].astype(F32)
        grads_ref[layer] = grads
        master = m_ref[...]
        tiles.append((grads + 5e-05 * master).astype(BF))
        moved.append((master - 0.1 * (0.9 * v_ref[...])).astype(BF))
        squares += [total_of(master * master), total_of(grads * grads)]
    tiles += moved
    rows = lax.broadcasted_iota(jnp.int32, (8, 128), 0)
    left = jnp.zeros((8, 128), F32)
    for at, square in enumerate(squares):
        left = jnp.where(rows == at, square, left)
    parts = []
    for _ in range(3):
        part = left.astype(BF)
        left = left - part.astype(F32)
        parts.append(part)
    tiles.append(jnp.concatenate(parts + [jnp.zeros((8, 128), BF)], axis=1))
    for z in range(8):
        for at, tile in enumerate(tiles):
            out_ref[z, at] = tile


def ring_squares_kernel(ring_ref, out_ref, low_ref, high_ref):
    total = jnp.zeros((8, 128), F32)
    for z in range(8):
        packed = ring_ref[z, 4].astype(F32)
        total = total + ((packed[:, :128] + packed[:, 128:256]) + packed[:, 256:384])
        half_ref = low_ref if z < 4 else high_ref
        half_ref[z % 4] = ring_ref[z, :4]
    out_ref[...] = jnp.broadcast_to(total[None], out_ref.shape)


def update_kernel(
    squares_ref,
    grads_ref,
    me_ref,
    mr_ref,
    ve_ref,
    vr_ref,
    *refs,
):
    low_refs, high_refs = refs[:4], refs[4:8]
    new_me_ref, new_mr_ref, new_ve_ref, new_vr_ref, low_work_ref, high_work_ref = refs[8:]
    squares = squares_ref[0]
    for peer in range(1, squares_ref.shape[0]):
        squares = squares + squares_ref[peer]
    norms = jnp.sqrt(squares)
    layers = (
        (me_ref, ve_ref, new_me_ref, new_ve_ref),
        (mr_ref, vr_ref, new_mr_ref, new_vr_ref),
    )
    for layer, (m_ref, v_ref, new_m_ref, new_v_ref) in enumerate(layers):
        wnorm = norms[2 * layer : 2 * layer + 1, :1]
        gnorm = norms[2 * layer + 1 : 2 * layer + 2, :1]
        trust = wnorm / (gnorm + 5e-05 * wnorm)
        master = m_ref[...]
        new_velocity = 0.9 * v_ref[...] + trust * (grads_ref[layer] + 5e-05 * master)
        new_v_ref[...] = new_velocity
        new_m_ref[...] = master - 0.1 * new_velocity
        for half_refs, work_ref in ((low_refs, low_work_ref), (high_refs, high_work_ref)):
            for s, half_ref in enumerate(half_refs):
                for z in range(4):
                    step = 0.1 * (trust * half_ref[z, layer].astype(F32))
                    work_ref[s, z, layer] = (half_ref[z, 2 + layer].astype(F32) - step).astype(BF)


def small_call(kernel, operands, outs, limit=16):
    whole = pl.BlockSpec(memory_space=pltpu.VMEM)
    moved = sum(x.size * x.dtype.itemsize for x in (*operands, *outs))
    return pl.pallas_call(
        kernel,
        out_shape=outs,
        in_specs=[whole] * len(operands),
        out_specs=[whole] * len(outs),
        compiler_params=pltpu.CompilerParams(vmem_limit_bytes=limit * 1024 * 1024),
        cost_estimate=pl.CostEstimate(flops=moved, bytes_accessed=moved, transcendentals=0),
    )(*operands)


def placements(at_ref, core, half, i, parts_ref, out_refs, sems):
    copies = []
    for j in range(4):
        x = lax.rem(at_ref[2] - (i if half else j) + 4, 4)
        y = lax.rem(at_ref[1] - j + 4, 4) if half else i
        for layer, out_ref in enumerate(out_refs):
            copies.append(
                pltpu.make_async_copy(
                    parts_ref.at[i, j, :, layer],
                    out_ref.at[pl.ds(half * 4, 4), y, core, x],
                    sems.at[half * 32 + i * 8 + j * 2 + layer],
                )
            )
    return copies


def place_kernel(other, halves, at_ref, *refs):
    expand_ref, reduce_ref, sems = refs[-3:]
    core = 1 - at_ref[0] if other else at_ref[0]
    copies = []
    for half, parts_ref in zip(halves, refs):
        for i in range(4):
            copies += placements(at_ref, core, half, i, parts_ref, (expand_ref, reduce_ref), sems)
    for copy in copies:
        copy.start()
    for copy in copies:
        copy.wait()


def place(other, halves, parts, into):
    _, _, z, _, r, n = parts[0].shape
    whole = jax.ShapeDtypeStruct((2 * z, 4, 2, 4, r, n), BF)
    hbm = pl.BlockSpec(memory_space=pl.ANY)
    at = jnp.stack([lax.axis_index(axis).astype(jnp.int32) for axis in ("c", "y", "x")])
    first = 1 + len(parts)
    return pl.pallas_call(
        functools.partial(place_kernel, other, halves),
        out_shape=(whole, whole),
        in_specs=[pl.BlockSpec(memory_space=pltpu.SMEM)]
        + [pl.BlockSpec(memory_space=pltpu.VMEM)] * len(parts)
        + [hbm] * len(into),
        out_specs=(hbm, hbm),
        scratch_shapes=[pltpu.SemaphoreType.DMA((64,))],
        input_output_aliases={first + at: at for at in range(len(into))},
        compiler_params=pltpu.CompilerParams(vmem_limit_bytes=8 * 1024 * 1024),
        cost_estimate=pl.CostEstimate(
            flops=parts[0].size, bytes_accessed=4 * len(parts) * parts[0].size, transcendentals=0
        ),
    )(at, *parts, *into)


def step(
    acts, saved_hidden, grad_out, master_reduce, master_expand, velocity_reduce, velocity_expand
):
    channels = grad_out.shape[1]
    middle = saved_hidden.shape[1]
    inv_c = 1.0 / float(channels) ** 0.5
    inv_m = 1.0 / float(middle) ** 0.5
    half = jax.ShapeDtypeStruct((16, 8, channels // 256, middle), BF)
    whole = pltpu.VMEM((channels, middle), BF)
    flops = 2 * grad_out.size * middle

    (cur,) = small_call(
        working_kernel,
        (master_expand, master_reduce),
        (jax.ShapeDtypeStruct((8, 2, *master_expand.shape), BF),),
        60,
    )
    along_z = exchange(cur, "z")
    mine = everywhere(along_z[:, 0], ("y", "x"))
    keep_e, send_e = local_call(
        functools.partial(expand_kernel, inv_m), (grad_out, saved_hidden), (half, half), [], flops
    )
    (sent_e,) = small_call(chip_sum_kernel, (keep_e, from_other_core(send_e)), (half,))
    other = from_other_core(mine)
    arrived_e = exchange(sent_e, ("y", "x"))
    grad_hidden, keep_r, send_r = local_call(
        functools.partial(hidden_kernel, inv_m, inv_c),
        (saved_hidden, mine, other),
        (jax.ShapeDtypeStruct(saved_hidden.shape, BF), half, half),
        [whole],
        2 * flops,
        (grad_out, acts),
    )
    (sent_r,) = small_call(chip_sum_kernel, (keep_r, from_other_core(send_r)), (half,))
    arrived_r = exchange(sent_r, ("y", "x"))
    row = lax.optimization_barrier(shifted(along_z[:, 1], "x"))
    plane_e = jnp.sum(arrived_e.astype(F32), axis=0).astype(BF)
    (over_plane,) = small_call(
        plane_sum_kernel,
        (plane_e, arrived_r),
        (jax.ShapeDtypeStruct((8, 2, channels // 256, middle), BF),),
    )
    arrived = exchange(over_plane, "z")
    mine_reduce = shifted(row, "y").reshape(half.shape)
    other_reduce = from_other_core(mine_reduce)
    (grad_in,) = local_call(
        functools.partial(back_kernel, inv_c),
        (grad_out, grad_hidden, mine_reduce, other_reduce),
        (jax.ShapeDtypeStruct(grad_out.shape, BF),),
        [whole],
        flops,
        limit=56,
    )

    state = (master_expand, master_reduce, velocity_expand, velocity_reduce)
    own = jax.ShapeDtypeStruct(master_expand.shape, F32)
    grads, rows = small_call(
        owner_kernel,
        (arrived, *state),
        (
            jax.ShapeDtypeStruct((2, *own.shape), F32),
            jax.ShapeDtypeStruct((8, 5, *own.shape), BF),
        ),
    )
    ring = exchange(rows, "z")
    quarter = jax.ShapeDtypeStruct((4, 4, *own.shape), BF)
    squares, low, high = small_call(
        ring_squares_kernel,
        (ring,),
        (jax.ShapeDtypeStruct((32, 8, 128), F32), quarter, quarter),
    )
    squares = exchange(squares, ("y", "c", "x"))
    lows = shifts(low, "x")
    highs = shifts(high, "y")
    four = jax.ShapeDtypeStruct((4, 4, 2, *own.shape), BF)
    new_me, new_mr, new_ve, new_vr, low_work, high_work = small_call(
        update_kernel,
        (squares, grads, *state, *lows, *highs),
        (own, own, own, own, four, four),
    )
    low_mine = everywhere(low_work, "y")
    high_mine = jnp.stack(shifts(high_work, "x"))
    low_other = from_other_core(low_mine)
    high_other = from_other_core(high_mine)
    placed = place(False, (0, 1), (low_mine, high_mine), ())
    placed = place(True, (0, 1), (low_other, high_other), placed)
    work_expand, work_reduce = (p.reshape(channels, middle) for p in placed)
    return (grad_in, new_mr, new_me, new_vr, new_ve, work_reduce, work_expand)


def solution(mesh):
    finer = Mesh(mesh.devices.reshape(8, 4, 2, 4), ROWS_OVER)
    split = P(ROWS_OVER, None)
    return jax.shard_map(
        step,
        mesh=finer,
        in_specs=(split,) * 7,
        out_specs=(split,) * 5 + (P(), P()),
        check_vma=False,
    )
```
